64 devices in a mesh: dp: 4 (over x, y), tp: 16 (over z, core).
Axes of the slice: x: 2, y: 2, z: 8, core: 2. Of those that a mesh axis runs over, the one named last changes fastest.
The devices are a block of a 4x4x8 slice.
Arguments:
- x_steps: bfloat16 [3, 384, 6144], P(None, 'dp'), parts along dimension 1
- seq_lens: int32 [384], P(('dp', 'tp')), parts along dimension 0
- k_cache: bfloat16 [384, 3072, 128], P(('dp', 'tp')), parts along dimension 0
- v_cache: bfloat16 [384, 3072, 128], P(('dp', 'tp')), parts along dimension 0
- ln_gain: bfloat16 [6144], replicated
- ln_bias: bfloat16 [6144], replicated
- w_q: bfloat16 [6144, 6144], P(None, 'tp')
- b_q: bfloat16 [6144], P('tp')
- w_kv: bfloat16 [6144, 256], replicated
- b_kv: bfloat16 [256], replicated
- w_out: bfloat16 [6144, 6144], P('tp')
- b_out: bfloat16 [6144], replicated
Outputs:
- output 1: bfloat16 [3, 384, 6144], P(None, 'dp'), parts along dimension 1
- output 2: bfloat16 [384, 3072, 128], P(('dp', 'tp')), parts along dimension 0
- output 3: bfloat16 [384, 3072, 128], P(('dp', 'tp')), parts along dimension 0
There are 4 independent parts. The reference program is written for one: setup_inputs(seed, part) draws one part's arguments, and reference() takes and returns one part's arrays. A program takes and returns all parts, laid end to end along the dimension named above; an argument that names none is the same for every part.
All inputs are finite; a program needn't handle non-finite values.
Results may differ from the reference program's by a relative error of at most 0.0120439.
Values are sent between devices in bfloat16 or wider.
A program may use at most 768 MiB of HBM per device.

```python
import jax
import jax.numpy as jnp
from jax import lax

BATCH_ROWS = 96
CACHE_LEN = 3072
D_MODEL = 6144
N_HEADS = 48
HEAD_DIM = 128
N_STEPS = 3
LN_EPS = 1e-5


def draw_lens(len_keys):
    seq_lens = jax.random.randint(len_keys[0], (BATCH_ROWS,), 64, CACHE_LEN - 3, dtype=jnp.int32)
    top_idx = jax.random.randint(len_keys[1], (), 0, BATCH_ROWS, dtype=jnp.int32)
    low_idx = (top_idx + 1 + jax.random.randint(len_keys[2], (), 0, BATCH_ROWS - 1, dtype=jnp.int32)) % BATCH_ROWS
    seq_lens = seq_lens.at[top_idx].set(CACHE_LEN - 4)
    return seq_lens.at[low_idx].set(64)


def setup_inputs(seed: int = 0, part: int = 0) -> dict:
    part_keys = jax.random.split(jax.random.fold_in(jax.random.key(seed), part), 4)
    shared_keys = jax.random.split(jax.random.key(seed + 1), 10)
    len_keys = jax.random.split(part_keys[0], 3)
    q_width = N_HEADS * HEAD_DIM
    cache_shape = (BATCH_ROWS, CACHE_LEN, HEAD_DIM)
    x_steps = jax.random.normal(part_keys[1], (N_STEPS, BATCH_ROWS, D_MODEL), jnp.float32)
    k_cache = 2.0 * jax.random.normal(part_keys[2], cache_shape, jnp.float32)
    v_cache = jax.random.normal(part_keys[3], cache_shape, jnp.float32)
    shared_dir = jax.random.normal(shared_keys[0], (HEAD_DIM,), jnp.float32)
    ln_gain = 1.0 + 0.3 * jax.random.normal(shared_keys[1], (D_MODEL,), jnp.float32)
    ln_bias = 0.3 * jax.random.normal(shared_keys[2], (D_MODEL,), jnp.float32)
    w_q = jax.random.normal(shared_keys[3], (D_MODEL, q_width), jnp.float32) * D_MODEL ** -0.5
    b_q = jnp.tile(shared_dir, N_HEADS) + 0.2 * jax.random.normal(shared_keys[4], (q_width,), jnp.float32)
    w_kv = jax.random.normal(shared_keys[5], (D_MODEL, 2 * HEAD_DIM), jnp.float32) * D_MODEL ** -0.5
    b_key = shared_dir + 0.2 * jax.random.normal(shared_keys[6], (HEAD_DIM,), jnp.float32)
    b_value = 0.3 * jax.random.normal(shared_keys[7], (HEAD_DIM,), jnp.float32)
    w_out = jax.random.normal(shared_keys[8], (q_width, D_MODEL), jnp.float32) * q_width ** -0.5
    b_out = 0.3 * jax.random.normal(shared_keys[9], (D_MODEL,), jnp.float32)
    return {
        'x_steps': x_steps.astype(jnp.bfloat16),
        'seq_lens': draw_lens(len_keys),
        'k_cache': k_cache.astype(jnp.bfloat16),
        'v_cache': v_cache.astype(jnp.bfloat16),
        'ln_gain': ln_gain.astype(jnp.bfloat16),
        'ln_bias': ln_bias.astype(jnp.bfloat16),
        'w_q': w_q.astype(jnp.bfloat16),
        'b_q': b_q.astype(jnp.bfloat16),
        'w_kv': w_kv.astype(jnp.bfloat16),
        'b_kv': jnp.concatenate([b_key, b_value]).astype(jnp.bfloat16),
        'w_out': w_out.astype(jnp.bfloat16),
        'b_out': b_out.astype(jnp.bfloat16),
    }


def layer_norm(x_rows, ln_gain, ln_bias):
    x_float = x_rows.astype(jnp.float32)
    row_mean = jnp.mean(x_float, axis=-1, keepdims=True)
    centered = x_float - row_mean
    row_var = jnp.mean(centered * centered, axis=-1, keepdims=True)
    scaled = centered * lax.rsqrt(row_var + LN_EPS)
    return (scaled * ln_gain.astype(jnp.float32) + ln_bias.astype(jnp.float32)).astype(jnp.bfloat16)


def attend_row(row_in):
    q_row, k_row, v_row, last_pos = row_in
    positions = jnp.arange(CACHE_LEN, dtype=jnp.int32)
    scores = jnp.einsum('hd,td->ht', q_row.astype(jnp.float32), k_row.astype(jnp.float32)) * HEAD_DIM ** -0.5
    scores = jnp.where(positions[None, :] <= last_pos, scores, -jnp.inf)
    weights = jnp.exp(scores - jnp.max(scores, axis=-1, keepdims=True))
    numerator = jnp.einsum('ht,td->hd', weights.astype(jnp.bfloat16).astype(jnp.float32), v_row.astype(jnp.float32))
    return (numerator / jnp.sum(weights, axis=-1, keepdims=True)).astype(jnp.bfloat16)


def reference(x_steps, seq_lens, k_cache, v_cache, ln_gain, ln_bias, w_q, b_q, w_kv, b_kv, w_out, b_out):
    positions = jnp.arange(CACHE_LEN, dtype=jnp.int32)

    def one_step(cache_pair, step_in):
        key_rows, value_rows = cache_pair
        x_rows, step_idx = step_in
        normed = layer_norm(x_rows, ln_gain, ln_bias)
        q_rows = (jnp.dot(normed, w_q, preferred_element_type=jnp.float32) + b_q.astype(jnp.float32)).astype(jnp.bfloat16)
        kv_rows = (jnp.dot(normed, w_kv, preferred_element_type=jnp.float32) + b_kv.astype(jnp.float32)).astype(jnp.bfloat16)
        write_pos = seq_lens + step_idx
        written = (positions[None, :] == write_pos[:, None])[:, :, None]
        key_rows = jnp.where(written, kv_rows[:, None, :HEAD_DIM], key_rows)
        value_rows = jnp.where(written, kv_rows[:, None, HEAD_DIM:], value_rows)
        attn_rows = lax.map(attend_row, (q_rows.reshape(BATCH_ROWS, N_HEADS, HEAD_DIM), key_rows, value_rows, write_pos))
        proj_sum = jnp.dot(attn_rows.reshape(BATCH_ROWS, N_HEADS * HEAD_DIM), w_out, preferred_element_type=jnp.float32)
        out_rows = (x_rows.astype(jnp.float32) + proj_sum + b_out.astype(jnp.float32)).astype(jnp.bfloat16)
        return (key_rows, value_rows), out_rows

    step_ids = jnp.arange(N_STEPS, dtype=jnp.int32)
    final_pair, y_steps = lax.scan(one_step, (k_cache, v_cache), (x_steps, step_ids))
    return y_steps, final_pair[0], final_pair[1]
```

```python
import functools

import jax
import jax.numpy as jnp
from jax import lax
from jax.experimental import pallas as pl
from jax.experimental.pallas import tpu as pltpu
from jax.sharding import PartitionSpec as P

LN_EPS = 1e-5
LANES = 128
PACK = 16
VMEM_LIMIT = 60 * 1024 * 1024
MESH = pl.DeviceIdType.MESH
F32 = jnp.float32
BF16 = jnp.bfloat16


def iota(shape, dim):
    return lax.broadcasted_iota(jnp.int32, shape, dim)


def one_hot(cond):
    return jnp.where(cond, 1.0, 0.0).astype(BF16)


def mm(a, b):
    return jnp.dot(a, b, preferred_element_type=F32)


def peer(index):
    return {'tp': index}


def enter(me, n):
    barrier = pltpu.get_barrier_semaphore()
    for k in range(1, n):
        pl.semaphore_signal(barrier, inc=1, device_id=peer(lax.rem(me + k, n)), device_id_type=MESH)
    return barrier


def pack_rows(src, source_row, n, rows, send_buf):
    total, width = src.shape
    heads = width // LANES
    rest = rows - PACK
    shape = (n * PACK, total)
    dest = iota(shape, 0) // PACK
    slot = iota(shape, 0) % PACK
    col = iota(shape, 1)
    send_buf[:, :width] = mm(one_hot(col == source_row(dest, slot)), src).astype(BF16)
    extra = jnp.zeros((n * PACK, LANES), F32)
    hit = col == source_row(dest, PACK + slot % rest)
    for head in range(heads):
        extra += mm(one_hot(hit & (slot // rest == head)), src[:, head * LANES:(head + 1) * LANES])
    send_buf[:, width:] = extra.astype(BF16)


def unpack_rows(recv_buf, total, width, place, rows):
    heads = width // LANES
    rest = rows - PACK
    shape = (total, recv_buf.shape[0])
    source, slot = place(iota(shape, 0))
    col = iota(shape, 1)
    main = mm(one_hot((slot < PACK) & (col == source * PACK + slot)), recv_buf[:, :width])
    tail = recv_buf[:, width:]
    extra = [
        mm(one_hot((slot >= PACK) & (col == source * PACK + head * rest + slot - PACK)), tail)
        for head in range(heads)
    ]
    return (main + jnp.concatenate(extra, axis=1)).astype(BF16)


def exchange(me, n, send_buf, recv_buf, send_sem, recv_sem):
    mine = pl.ds(pl.multiple_of(me * PACK, PACK), PACK)
    copies = []
    order = sorted(range(1, n), key=lambda k: -min(k, n - k))
    for k in order:
        dest = lax.rem(me + k, n)
        copy = pltpu.make_async_remote_copy(
            src_ref=send_buf.at[pl.ds(pl.multiple_of(dest * PACK, PACK), PACK)],
            dst_ref=recv_buf.at[mine],
            send_sem=send_sem.at[k],
            recv_sem=recv_sem.at[k],
            device_id=peer(dest),
            device_id_type=MESH,
        )
        copy.start()
        copies.append(copy)
    recv_buf[mine] = send_buf[mine]
    return copies


def query_kernel(n, x_hbm, gain_ref, bias_ref, wq_hbm, bq_ref, wkv_hbm, bkv_ref, q_ref, kv_ref,
                 x_v, h_v, wq_v, wkv_v, acc, kv_acc, send_buf, recv_buf,
                 x_sem, wq_sem, wkv_sem, send_sem, recv_sem):
    me = lax.axis_index('tp')
    steps, group, width = x_v.shape
    q_cols = wq_v.shape[1]
    total = steps * group
    local = group // n
    rows = local * steps
    heads = q_cols // LANES
    barrier = enter(me, n)
    x_copies = []
    for s in range(steps):
        x_copies.append(pltpu.make_async_copy(x_hbm.at[s], x_v.at[s], x_sem.at[s]))
        x_copies[-1].start()
    wq_copy = pltpu.make_async_copy(wq_hbm, wq_v, wq_sem)
    wq_copy.start()
    wkv_copy = pltpu.make_async_copy(wkv_hbm, wkv_v, wkv_sem)
    wkv_copy.start()

    for s in range(steps):
        x_copies[s].wait()

        @pl.loop(0, group // PACK)
        def _(r):
            at = pl.ds(pl.multiple_of(r * PACK, PACK), PACK)
            x = x_v[s, at, :].astype(F32)
            mean = jnp.mean(x, axis=-1, keepdims=True)
            centered = x - mean
            var = jnp.mean(centered * centered, axis=-1, keepdims=True)
            scaled = centered * lax.rsqrt(var + LN_EPS)
            h = (scaled * gain_ref[...].astype(F32) + bias_ref[...].astype(F32)).astype(BF16)
            h_v[pl.ds(pl.multiple_of(s * group + r * PACK, PACK), PACK), :] = h

    depth = width // 8
    wq_copy.wait()
    acc[...] = jnp.zeros_like(acc)

    @pl.loop(0, width // depth)
    def _(c):
        at = pl.ds(pl.multiple_of(c * depth, depth), depth)
        acc[...] += mm(h_v[:, at], wq_v[at, :])

    q = (acc[...] + bq_ref[...].astype(F32)).astype(BF16)
    pack_rows(q, lambda dest, r: (r % steps) * group + dest * local + r // steps, n, rows, send_buf)
    pl.semaphore_wait(barrier, n - 1)
    copies = exchange(me, n, send_buf, recv_buf, send_sem, recv_sem)

    wkv_copy.wait()
    kv_acc[...] = jnp.zeros_like(kv_acc)

    @pl.loop(0, width // depth)
    def _(c):
        at = pl.ds(pl.multiple_of(c * depth, depth), depth)
        kv_acc[...] += mm(h_v[:, at], wkv_v[at, :])

    kv = (kv_acc[...] + bkv_ref[...].astype(F32)).astype(BF16)
    pad = kv_ref.shape[1]
    shape = (local * pad, total)
    row = iota(shape, 0)
    own = one_hot((row % pad < steps) & (iota(shape, 1) == (row % pad) * group + me * local + row // pad))
    kv_ref[...] = mm(own, kv).astype(F32).reshape(kv_ref.shape)

    for copy in copies:
        copy.wait()
    per_seq = n * steps
    q_all = unpack_rows(
        recv_buf, total, q_cols,
        lambda row: ((row % per_seq) // steps, (row // per_seq) * steps + row % steps), rows)
    for i in range(local):
        for head in range(heads):
            q_ref[i, head * per_seq:(head + 1) * per_seq, :] = q_all[
                i * per_seq:(i + 1) * per_seq, head * LANES:(head + 1) * LANES]


def attend_kernel(steps, block, lens_ref, q_ref, kv_ref, k_ref, v_ref, o_ref, ko_ref, vo_ref, scores):
    seq_len = lens_ref[pl.program_id(0)]
    n_rows, head_dim = q_ref.shape[1:]
    cache_len = k_ref.shape[1]
    window = 2 * PACK
    ko_ref[...] = k_ref[...]
    vo_ref[...] = v_ref[...]
    start = jnp.minimum((seq_len // PACK) * PACK, cache_len - window)
    at = pl.ds(pl.multiple_of(start, PACK), window)
    pos = iota((window, head_dim), 0) + start
    k_win = ko_ref[0, at, :].astype(F32)
    v_win = vo_ref[0, at, :].astype(F32)
    for s in range(steps):
        k_win = jnp.where(pos == seq_len + s, kv_ref[0, s:s + 1, :head_dim], k_win)
        v_win = jnp.where(pos == seq_len + s, kv_ref[0, s:s + 1, head_dim:], v_win)
    ko_ref[0, at, :] = k_win.astype(BF16)
    vo_ref[0, at, :] = v_win.astype(BF16)

    n_blocks = (seq_len + steps + block - 1) // block
    factor = head_dim ** -0.5 * 1.4426950408889634
    last = seq_len + iota((n_rows, block), 0) % steps
    col = iota((n_rows, block), 1)
    q = q_ref[0]

    def fold(value, op):
        out = value[:, :LANES]
        for c in range(1, block // LANES):
            out = op(out, value[:, c * LANES:(c + 1) * LANES])
        return out

    def first(j, top):
        at = pl.ds(pl.multiple_of(j * block, block), block)
        t = lax.dot_general(q, ko_ref[0, at, :], (((1,), (1,)), ((), ())), preferred_element_type=F32)
        t = jnp.where(col <= last - j * block, t, -jnp.inf)
        scores[:, at] = t
        return jnp.maximum(top, fold(t, jnp.maximum))

    top = lax.fori_loop(0, n_blocks, first, jnp.full((n_rows, LANES), -jnp.inf, F32))
    top = jnp.max(top, axis=-1, keepdims=True)

    def second(j, carry):
        den, num = carry
        at = pl.ds(pl.multiple_of(j * block, block), block)
        p = jnp.exp2((scores[:, at] - top) * factor)
        num = num + mm(p.astype(BF16), vo_ref[0, at, :])
        return den + fold(p, jnp.add), num

    zero = jnp.zeros((n_rows, LANES), F32)
    den, num = lax.fori_loop(0, n_blocks, second, (zero, zero))
    out = (num / jnp.sum(den, axis=-1, keepdims=True)).astype(BF16)
    per_seq = o_ref.shape[1]
    for head in range(n_rows // per_seq):
        o_ref[0, :, head * LANES:(head + 1) * LANES] = out[head * per_seq:(head + 1) * per_seq]


def project_kernel(n, steps, o_ref, x_hbm, wo_hbm, bo_hbm, y_hbm,
                   a_v, wo_v, x_v, bo_v, part, pair_send, pair_recv, rs_send, rs_recv, y_v, send_buf, recv_buf,
                   wo_sem, in_sem, a_send, a_recv, pair_ssem, pair_rsem, rs_ssem, rs_rsem, ag_ssem, ag_rsem,
                   d2d_ssem, d2d_rsem, out_sem):
    me = lax.axis_index('tp')
    total, depth = a_v.shape
    cols = wo_v.shape[2]
    chips = n // 2
    far = chips // 2
    chip = me // 2
    core = me % 2
    mate = me + 1 - 2 * core
    group = total // steps
    local = group // n
    rows = local * steps
    per_seq = n * steps
    half = total // 2
    barrier = enter(me, n)

    def block_at(index):
        return pl.ds(pl.multiple_of(index * cols, LANES), cols)

    def half_at(h):
        return pl.ds(h * half, half)

    offsets = [far]
    for k in range(far - 1, 0, -1):
        offsets += [k, chips - k]
    offsets.append(0)
    wo_copies = []
    for pos, off in enumerate(offsets):
        dest = lax.rem(chip + off, chips)
        for side, dev in enumerate((2 * dest + 1 - core, 2 * dest + core)):
            copy = pltpu.make_async_copy(wo_hbm.at[:, block_at(dev)], wo_v.at[2 * pos + side], wo_sem.at[2 * pos + side])
            copy.start()
            wo_copies.append(copy)
    x_copy = pltpu.make_async_copy(x_hbm.at[:, block_at(me)], x_v, in_sem.at[0])
    x_copy.start()
    bo_copy = pltpu.make_async_copy(bo_hbm.at[:, block_at(me)], bo_v, in_sem.at[1])
    bo_copy.start()

    pack_rows(o_ref[...], lambda dest, r: (r // steps) * per_seq + dest * steps + r % steps, n, rows, send_buf)
    pl.semaphore_wait(barrier, n - 1)
    copies = exchange(me, n, send_buf, recv_buf, a_send, a_recv)
    for copy in copies:
        copy.wait()
    a_v[...] = unpack_rows(
        recv_buf, total, depth,
        lambda row: ((row % group) // local, (row % local) * steps + row // group), rows)

    pair_copies = {}

    def multiply(off):
        pos = offsets.index(off)
        wo_copies[2 * pos].wait()
        pair_send[pos] = mm(a_v[...], wo_v[2 * pos]).astype(BF16)
        copy = pltpu.make_async_remote_copy(
            src_ref=pair_send.at[pos], dst_ref=pair_recv.at[pos], send_sem=pair_ssem.at[pos],
            recv_sem=pair_rsem.at[pos], device_id=peer(mate), device_id_type=MESH)
        copy.start()
        pair_copies[off] = copy
        wo_copies[2 * pos + 1].wait()
        part[pos] = mm(a_v[...], wo_v[2 * pos + 1])

    arrived = set()

    def chip_sum(off, h):
        pos = offsets.index(off)
        if off not in arrived:
            pair_copies[off].wait_recv()
            arrived.add(off)
        return part[pos, half_at(h), :] + pair_recv[pos, half_at(h), :].astype(F32)

    sign = (-1, 1)
    plan = [[(far, d)] + [(k, h) for k in range(far - 1, 0, -1) for h in (1 - d, d)] for d in (0, 1)]
    n_slots = len(plan[0])
    nexts = [2 * lax.rem(chip + chips + sign[d], chips) + core for d in (0, 1)]
    rs_copies = [[], []]

    def reduce_slot(d, slot):
        k, h = plan[d][slot]
        value = chip_sum((sign[d] * k) % chips, h)
        if slot >= 2:
            rs_copies[d][slot - 2].wait_recv()
            value = value + rs_recv[d, slot - 2].astype(F32)
        rs_send[d, slot] = value.astype(BF16)
        copy = pltpu.make_async_remote_copy(
            src_ref=rs_send.at[d, slot], dst_ref=rs_recv.at[d, slot], send_sem=rs_ssem.at[d, slot],
            recv_sem=rs_rsem.at[d, slot], device_id=peer(nexts[d]), device_id_type=MESH)
        copy.start()
        rs_copies[d].append(copy)

    todo = list(offsets)
    multiply(todo.pop(0))
    multiply(todo.pop(0))
    for slot in range(n_slots):
        for d in (0, 1):
            need = (sign[d] * plan[d][slot][0]) % chips
            while need in todo:
                multiply(todo.pop(0))
            reduce_slot(d, slot)
        for _ in range(2):
            if todo:
                multiply(todo.pop(0))

    x_copy.wait()
    bo_copy.wait()
    for d in (0, 1):
        rs_copies[d][n_slots - 2].wait_recv()
        rs_copies[d][n_slots - 1].wait_recv()
    own = 2 * chip + core
    for h in (0, 1):
        value = chip_sum(0, h)
        for d in (0, 1):
            slot = n_slots - 1 if h == d else n_slots - 2
            value = value + rs_recv[d, slot].astype(F32)
        value = x_v[half_at(h), :].astype(F32) + value + bo_v[...].astype(F32)
        y_v[own, half_at(h), :] = value.astype(BF16)

    d2d_copies = []
    out_copies = []

    def spread(index, hop, h):
        at = y_v.at[index, half_at(h)]
        pos = 2 * hop + h
        copy = pltpu.make_async_remote_copy(
            src_ref=at, dst_ref=at, send_sem=d2d_ssem.at[pos], recv_sem=d2d_rsem.at[pos],
            device_id=peer(mate), device_id_type=MESH)
        copy.start()
        other = index + 1 - 2 * core
        d2d_copies.append((copy, other, h, pos))
        out = pltpu.make_async_copy(at, y_hbm.at[half_at(h), block_at(index)], out_sem.at[0, pos])
        out.start()
        out_copies.append(out)

    ag_copies = [[], []]

    def gather_slot(d, slot, index, h):
        at = y_v.at[index, half_at(h)]
        copy = pltpu.make_async_remote_copy(
            src_ref=at, dst_ref=at, send_sem=ag_ssem.at[d, slot], recv_sem=ag_rsem.at[d, slot],
            device_id=peer(nexts[d]), device_id_type=MESH)
        copy.start()
        ag_copies[d].append(copy)

    for j in (0, 1):
        for d in (0, 1):
            gather_slot(d, j, own, 1 - d if j == 0 else d)
    for h in (0, 1):
        spread(own, 0, h)
    for slot in range(n_slots):
        back = slot // 2 + 1
        for d in (0, 1):
            h = 1 - d if slot % 2 == 0 else d
            hop = (-sign[d] * back) % chips
            index = 2 * lax.rem(chip + hop, chips) + core
            ag_copies[d][slot].wait_recv()
            if slot + 2 < n_slots:
                gather_slot(d, slot + 2, index, h)
            spread(index, hop, h)
    for copy, other, h, pos in d2d_copies:
        copy.wait_recv()
        out = pltpu.make_async_copy(
            y_v.at[other, half_at(h)], y_hbm.at[half_at(h), block_at(other)], out_sem.at[1, pos])
        out.start()
        out_copies.append(out)
    for copy in pair_copies.values():
        copy.wait_send()
    for d in (0, 1):
        for copy in rs_copies[d] + ag_copies[d]:
            copy.wait_send()
    for copy, _, _, _ in d2d_copies:
        copy.wait_send()
    for out in out_copies:
        out.wait()


def solution(mesh):
    n = mesh.shape['tp']
    vmem = pl.BlockSpec(memory_space=pltpu.VMEM)
    anywhere = pl.BlockSpec(memory_space=pl.ANY)
    dma = pltpu.SemaphoreType.DMA

    def local_block(x_steps, seq_lens, k_cache, v_cache, ln_gain, ln_bias, w_q, b_q, w_kv, b_kv, w_out, b_out):
        steps, group, width = x_steps.shape
        local, cache_len, head_dim = k_cache.shape
        total = steps * group
        q_cols = w_q.shape[1]
        kv_cols = w_kv.shape[1]
        heads = q_cols // head_dim
        per_seq = n * steps
        pad = 8
        q_rows, kv_rows = pl.pallas_call(
            functools.partial(query_kernel, n),
            name='query',
            out_shape=(
                jax.ShapeDtypeStruct((local, heads * per_seq, head_dim), BF16),
                jax.ShapeDtypeStruct((local, pad, kv_cols), F32),
            ),
            in_specs=[anywhere, vmem, vmem, anywhere, vmem, anywhere, vmem],
            out_specs=(vmem, vmem),
            scratch_shapes=[
                pltpu.VMEM((steps, group, width), BF16),
                pltpu.VMEM((total, width), BF16),
                pltpu.VMEM((width, q_cols), BF16),
                pltpu.VMEM((width, kv_cols), BF16),
                pltpu.VMEM((total, q_cols), F32),
                pltpu.VMEM((total, kv_cols), F32),
                pltpu.VMEM((n * PACK, q_cols + LANES), BF16),
                pltpu.VMEM((n * PACK, q_cols + LANES), BF16),
                dma((steps,)), dma, dma, dma((n,)), dma((n,)),
            ],
            compiler_params=pltpu.CompilerParams(
                collective_id=0, has_side_effects=True, vmem_limit_bytes=VMEM_LIMIT),
        )(x_steps, ln_gain[None], ln_bias[None], w_q, b_q[None], w_kv, b_kv[None])

        block = cache_len // 3 if cache_len % (3 * LANES) == 0 else cache_len
        per_row = lambda i, lens: (i, 0, 0)
        out_heads, k_out, v_out = pl.pallas_call(
            functools.partial(attend_kernel, steps, block),
            name='attend',
            out_shape=(
                jax.ShapeDtypeStruct((local, per_seq, q_cols), BF16),
                jax.ShapeDtypeStruct(k_cache.shape, BF16),
                jax.ShapeDtypeStruct(v_cache.shape, BF16),
            ),
            grid_spec=pltpu.PrefetchScalarGridSpec(
                num_scalar_prefetch=1,
                grid=(local,),
                in_specs=[
                    pl.BlockSpec((1, heads * per_seq, head_dim), per_row),
                    pl.BlockSpec((1, pad, kv_cols), per_row),
                    pl.BlockSpec((1, cache_len, head_dim), per_row),
                    pl.BlockSpec((1, cache_len, head_dim), per_row),
                ],
                out_specs=(
                    pl.BlockSpec((1, per_seq, q_cols), per_row),
                    pl.BlockSpec((1, cache_len, head_dim), per_row),
                    pl.BlockSpec((1, cache_len, head_dim), per_row),
                ),
                scratch_shapes=[pltpu.VMEM((heads * per_seq, cache_len), F32)],
            ),
            compiler_params=pltpu.CompilerParams(vmem_limit_bytes=VMEM_LIMIT),
        )(seq_lens, q_rows, kv_rows, k_cache, v_cache)

        cols = width // n
        chips = n // 2
        n_slots = chips - 1
        half = total // 2
        y = pl.pallas_call(
            functools.partial(project_kernel, n, steps),
            name='project',
            out_shape=jax.ShapeDtypeStruct((total, width), BF16),
            in_specs=[vmem, anywhere, anywhere, anywhere],
            out_specs=anywhere,
            scratch_shapes=[
                pltpu.VMEM((total, q_cols), BF16),
                pltpu.VMEM((n, q_cols, cols), BF16),
                pltpu.VMEM((total, cols), BF16),
                pltpu.VMEM((1, cols), BF16),
                pltpu.VMEM((chips, total, cols), F32),
                pltpu.VMEM((chips, total, cols), BF16),
                pltpu.VMEM((chips, total, cols), BF16),
                pltpu.VMEM((2, n_slots, half, cols), BF16),
                pltpu.VMEM((2, n_slots, half, cols), BF16),
                pltpu.VMEM((n, total, cols), BF16),
                pltpu.VMEM((n * PACK, q_cols + LANES), BF16),
                pltpu.VMEM((n * PACK, q_cols + LANES), BF16),
                dma((n,)), dma((2,)), dma((n,)), dma((n,)), dma((chips,)), dma((chips,)),
                dma((2, n_slots)), dma((2, n_slots)), dma((2, n_slots)), dma((2, n_slots)),
                dma((2 * chips,)), dma((2 * chips,)), dma((2, 2 * chips)),
            ],
            compiler_params=pltpu.CompilerParams(
                collective_id=1, has_side_effects=True, vmem_limit_bytes=VMEM_LIMIT),
        )(out_heads.reshape(total, q_cols), x_steps.reshape(total, width), w_out, b_out[None])
        return y.reshape(x_steps.shape), k_out, v_out

    row_spec = P(('dp', 'tp'), None, None)
    return jax.shard_map(
        local_block,
        mesh=mesh,
        in_specs=(P(None, 'dp', None), P(('dp', 'tp')), row_spec, row_spec, P(None), P(None), P(None, 'tp'), P('tp'), P(None, None), P(None), P('tp', None), P(None)),
        out_specs=(P(None, 'dp', None), row_spec, row_spec),
        check_vma=False,
    )
```

```python
import functools

import jax
import jax.numpy as jnp
from jax import lax
from jax.experimental import pallas as pl
from jax.experimental.pallas import tpu as pltpu
from jax.sharding import PartitionSpec as P

LN_EPS = 1e-5
LANES = 128
PACK = 16
PARTS = 2
VMEM_LIMIT = 60 * 1024 * 1024
MESH = pl.DeviceIdType.MESH
F32 = jnp.float32
BF16 = jnp.bfloat16


def iota(shape, dim):
    return lax.broadcasted_iota(jnp.int32, shape, dim)


def one_hot(rows, cols, index, valid=None):
    at = index if valid is None else jnp.where(valid, index, -1)
    return jnp.where(iota((rows, cols), 1) == at, 1.0, 0.0).astype(BF16)


def mm(a, b):
    return jnp.dot(a, b, preferred_element_type=F32)


def peer(index):
    return {'tp': index}


def tiles_of(head, rows):
    return range(head * rows // PACK, ((head + 1) * rows - 1) // PACK + 1)


def pack_rows(src, source_row, n, rows, send_buf):
    total, width = src.shape
    heads = width // LANES
    p = iota((n * PACK, 1), 0)
    dest, slot = p // PACK, p % PACK
    for tile in range(send_buf.shape[-1] // LANES):
        unit = tile * PACK + slot
        index = source_row(dest, unit % rows)
        value = jnp.zeros((n * PACK, LANES), F32)
        for head in range(heads):
            if tile in tiles_of(head, rows):
                hot = one_hot(n * PACK, total, index, unit // rows == head)
                value += mm(hot, src[:, head * LANES:(head + 1) * LANES])
        send_buf[:, tile * LANES:(tile + 1) * LANES] = value.astype(BF16)


def unpack_rows(recv_buf, total, heads, place, rows):
    source, row = place(iota((total, 1), 0))
    out = []
    for head in range(heads):
        unit = head * rows + row
        value = jnp.zeros((total, LANES), F32)
        for tile in tiles_of(head, rows):
            hot = one_hot(total, recv_buf.shape[0], source * PACK + unit % PACK, unit // PACK == tile)
            value += mm(hot, recv_buf[:, tile * LANES:(tile + 1) * LANES])
        out.append(value.astype(BF16))
    return out


def spread_row(row_ref, src_ref):
    for j in range(src_ref.shape[0]):
        row_ref[:, j * LANES:(j + 1) * LANES] = src_ref[j:j + 1, :].astype(F32)


def local_kernel(n, lens_ref, x_hbm, gain_ref, bias_ref, wq_hbm, bq_ref, wkv_hbm, bkv_ref, k_hbm, v_hbm,
                 pieces_ref, ko_hbm, vo_hbm,
                 x_v, h_v, wq_v, wkv_v, k_v, v_v, acc, kv_acc, gain_v, bias_v, bq_v, bkv_v, fresh,
                 x_sem, w_sem, in_sem, out_sem):
    me = lax.axis_index('tp')
    steps, group, width = x_v.shape
    q_cols = wq_v.shape[1]
    total = steps * group
    local, cache_len, head_dim = k_v.shape
    x_copies = [pltpu.make_async_copy(x_hbm.at[s], x_v.at[s], x_sem.at[s]) for s in range(steps)]
    wkv_copy = pltpu.make_async_copy(wkv_hbm, wkv_v, w_sem.at[0])
    wq_copy = pltpu.make_async_copy(wq_hbm, wq_v, w_sem.at[1])
    caches = ((k_hbm, k_v, ko_hbm), (v_hbm, v_v, vo_hbm))
    ins = [[pltpu.make_async_copy(src.at[i], mid.at[i], in_sem.at[c, i]) for i in range(local)]
           for c, (src, mid, _) in enumerate(caches)]
    outs = [[pltpu.make_async_copy(mid.at[i], dst.at[i], out_sem.at[c, i]) for i in range(local)]
            for c, (_, mid, dst) in enumerate(caches)]
    for copy in x_copies + [wkv_copy] + ins[0] + ins[1] + [wq_copy]:
        copy.start()
    spread_row(gain_v, gain_ref)
    spread_row(bias_v, bias_ref)
    spread_row(bq_v, bq_ref)
    spread_row(bkv_v, bkv_ref)

    for s in range(steps):
        x_copies[s].wait()

        @pl.loop(0, group // PACK)
        def _(r):
            at = pl.ds(pl.multiple_of(r * PACK, PACK), PACK)
            x = x_v[s, at, :].astype(F32)
            mean = jnp.mean(x, axis=-1, keepdims=True)
            centered = x - mean
            var = jnp.mean(centered * centered, axis=-1, keepdims=True)
            scaled = centered * lax.rsqrt(var + LN_EPS)
            h = (scaled * gain_v[...] + bias_v[...]).astype(BF16)
            h_v[pl.ds(pl.multiple_of(s * group + r * PACK, PACK), PACK), :] = h

    depth = width // 8

    def product(total_ref, w_v):
        total_ref[...] = jnp.zeros_like(total_ref)

        @pl.loop(0, width // depth)
        def _(c):
            at = pl.ds(pl.multiple_of(c * depth, depth), depth)
            total_ref[...] += mm(h_v[:, at], w_v[at, :])

    wkv_copy.wait()
    product(kv_acc, wkv_v)
    kv = (kv_acc[...] + bkv_v[...]).astype(BF16)
    pad = fresh.shape[0] // local
    row = iota((local * pad, 1), 0)
    fresh[...] = mm(one_hot(local * pad, total, (row % pad) * group + me * local + row // pad, row % pad < steps), kv)
    window = 2 * PACK
    for c in (0, 1):
        for i in range(local):
            mid = caches[c][1]
            seq_len = lens_ref[i]
            start = jnp.minimum((seq_len // PACK) * PACK, cache_len - window)
            at = pl.ds(pl.multiple_of(start, PACK), window)
            pos = iota((window, head_dim), 0) + start
            ins[c][i].wait()
            value = mid[i, at, :].astype(F32)
            for s in range(steps):
                new = fresh[i * pad + s:i * pad + s + 1, c * head_dim:(c + 1) * head_dim]
                value = jnp.where(pos == seq_len + s, new, value)
            mid[i, at, :] = value.astype(BF16)
            outs[c][i].start()

    wq_copy.wait()
    product(acc, wq_v)
    q = (acc[...] + bq_v[...]).astype(BF16)
    share = local // PARTS
    for part in range(PARTS):
        pack_rows(
            q, lambda dest, r: (r % steps) * group + dest * local + part * share + r // steps,
            n, share * steps, pieces_ref.at[part])
    for c in (0, 1):
        for copy in outs[c]:
            copy.wait()


def group_kernel(n, steps, block, lens_ref, pieces_hbm, k_hbm, v_hbm, x_hbm, wo_hbm, bo_ref, y_hbm,
                 pieces_v, q_recv, q_v, k_v, v_v, scores, heads_v, o_send, o_recv, a_v, wo_v, x_v, rest_v, bo_v,
                 part_v, pair_send, pair_recv, rs_send, rs_recv, y_v,
                 in_sem, k_sem, v_sem, wo_sem, q_ssem, q_rsem, o_ssem, o_rsem, pair_ssem, pair_rsem,
                 rs_ssem, rs_rsem, ag_ssem, ag_rsem, d2d_ssem, d2d_rsem, out_sem):
    me = lax.axis_index('tp')
    local, cache_len, head_dim = k_v.shape
    share = local // PARTS
    rows = share * steps
    per_seq = n * steps
    total = share * per_seq
    depth = a_v.shape[2]
    heads = depth // head_dim
    cols = wo_v.shape[2]
    chips = n // 2
    far = chips // 2
    chip = me // 2
    core = me % 2
    mate = me + 1 - 2 * core
    group = local * n

    barrier = pltpu.get_barrier_semaphore()
    for k in range(1, n):
        pl.semaphore_signal(barrier, inc=1, device_id=peer(lax.rem(me + k, n)), device_id_type=MESH)

    def block_at(index):
        return pl.ds(pl.multiple_of(index * cols, LANES), cols)

    pieces_copy = pltpu.make_async_copy(pieces_hbm, pieces_v, in_sem.at[0])
    pieces_copy.start()
    x_copy = pltpu.make_async_copy(x_hbm.at[:, block_at(me)], x_v, in_sem.at[1])
    x_copy.start()

    cache_in = [(pltpu.make_async_copy(k_hbm.at[i], k_v.at[i], k_sem.at[i]),
                 pltpu.make_async_copy(v_hbm.at[i], v_v.at[i], v_sem.at[i])) for i in range(local)]
    for k_copy, v_copy in cache_in:
        k_copy.start()
        v_copy.start()
    offsets = [far]
    for k in range(far - 1, 0, -1):
        offsets += [k, chips - k]
    offsets.append(0)
    wo_copies = []
    for pos, off in enumerate(offsets):
        dest = lax.rem(chip + off, chips)
        for side, dev in enumerate((2 * dest + 1 - core, 2 * dest + core)):
            copy = pltpu.make_async_copy(wo_hbm.at[:, block_at(dev)], wo_v.at[2 * pos + side], wo_sem.at[2 * pos + side])
            copy.start()
            wo_copies.append(copy)

    bo_v[...] = bo_ref[...].astype(F32)
    tiles = cols // LANES
    bias = jnp.concatenate([bo_v[pl.ds(me * tiles + j, 1), :] for j in range(tiles)], axis=1)
    x_copy.wait()
    row = iota((total, 1), 0)
    for part in range(PARTS):
        source = (row // (n * share)) * group + ((row // share) % n) * local + part * share + row % share
        rest_v[part] = mm(one_hot(total, steps * group, source), x_v[...]) + bias

    def exchange(part, send_buf, recv_buf, send_sem, recv_sem):
        mine = pl.ds(pl.multiple_of(me * PACK, PACK), PACK)
        copies = []
        for k in sorted(range(1, n), key=lambda k: -min(k, n - k)):
            dest = lax.rem(me + k, n)
            copy = pltpu.make_async_remote_copy(
                src_ref=send_buf.at[part, pl.ds(pl.multiple_of(dest * PACK, PACK), PACK)],
                dst_ref=recv_buf.at[part, mine],
                send_sem=send_sem.at[part, k], recv_sem=recv_sem.at[part, k],
                device_id=peer(dest), device_id_type=MESH)
            copy.start()
            copies.append(copy)
        recv_buf[part, mine] = send_buf[part, mine]
        return copies

    pieces_copy.wait()
    pl.semaphore_wait(barrier, n - 1)
    q_copies = [exchange(part, pieces_v, q_recv, q_ssem, q_rsem) for part in range(PARTS)]

    n_rows = heads * per_seq
    factor = head_dim ** -0.5 * 1.4426950408889634
    col_step = iota((n_rows, block), 1) - iota((n_rows, block), 0) % steps

    def fold(value, op):
        out = value[:, :LANES]
        for c in range(1, block // LANES):
            out = op(out, value[:, c * LANES:(c + 1) * LANES])
        return out

    def attend(part):
        for copy in q_copies[part]:
            copy.wait_recv()
        by_head = unpack_rows(
            q_recv.at[part], total, heads,
            lambda row: ((row % per_seq) // steps, (row // per_seq) * steps + row % steps), rows)
        for i in range(share):
            for head in range(heads):
                q_v[i, head * per_seq:(head + 1) * per_seq, :] = by_head[head][i * per_seq:(i + 1) * per_seq]

        for copy in cache_in[part * share:(part + 1) * share]:
            copy[0].wait()
            copy[1].wait()

        @pl.loop(0, share)
        def _(i):
            seq = part * share + i
            seq_len = lens_ref[seq]
            q = q_v[i]
            top = jnp.full((n_rows, LANES), -jnp.inf, F32)
            for j in range(cache_len // block):
                at = slice(j * block, (j + 1) * block)
                t = lax.dot_general(q, k_v[seq, at, :], (((1,), (1,)), ((), ())), preferred_element_type=F32)
                t = jnp.where(col_step <= seq_len - j * block, t, -jnp.inf)
                scores[:, at] = t
                top = jnp.maximum(top, fold(t, jnp.maximum))
            top = jnp.max(top, axis=-1, keepdims=True)
            den = jnp.zeros((n_rows, LANES), F32)
            num = jnp.zeros((n_rows, head_dim), F32)
            for j in range(cache_len // block):
                at = slice(j * block, (j + 1) * block)
                p = jnp.exp2((scores[:, at] - top) * factor)
                num = num + mm(p.astype(BF16), v_v[seq, at, :])
                den = den + fold(p, jnp.add)
            out = (num / jnp.sum(den, axis=-1, keepdims=True)).astype(BF16)
            to = pl.ds(pl.multiple_of(i * per_seq, PACK), per_seq)
            for head in range(heads):
                heads_v[to, head * LANES:(head + 1) * LANES] = out[head * per_seq:(head + 1) * per_seq]

        pack_rows(
            heads_v[...], lambda dest, r: (r // steps) * per_seq + dest * steps + r % steps, n, rows, o_send.at[part])
        return exchange(part, o_send, o_recv, o_ssem, o_rsem)

    o_copies = [attend(part) for part in range(PARTS)]

    cut = (total // 2 + PACK - 1) // PACK * PACK
    halves = (pl.ds(0, cut), pl.ds(cut, total - cut))
    sign = (-1, 1)
    nexts = [2 * lax.rem(chip + chips + sign[d], chips) + core for d in (0, 1)]
    own = 2 * chip + core
    pair_copies = {}
    arrived = set()
    rs_copies = {}
    ag_copies = {}
    d2d_copies = []
    out_copies = []
    todo = {part: list(offsets) for part in range(PARTS)}

    def collect(part):
        for copy in o_copies[part]:
            copy.wait_recv()
        by_head = unpack_rows(
            o_recv.at[part], total, heads,
            lambda row: ((row // share) % n, (row % share) * steps + row // (n * share)), rows)
        for head in range(heads):
            a_v[part, :, head * LANES:(head + 1) * LANES] = by_head[head]

    def multiply(part, off):
        todo[part].remove(off)
        pos = offsets.index(off)
        if part == 0:
            wo_copies[2 * pos].wait()
        pair_send[part, pos] = mm(a_v[part], wo_v[2 * pos]).astype(BF16)
        copy = pltpu.make_async_remote_copy(
            src_ref=pair_send.at[part, pos], dst_ref=pair_recv.at[part, pos], send_sem=pair_ssem.at[part, pos],
            recv_sem=pair_rsem.at[part, pos], device_id=peer(mate), device_id_type=MESH)
        copy.start()
        pair_copies[part, off] = copy
        if part == 0:
            wo_copies[2 * pos + 1].wait()
        part_v[part, pos] = mm(a_v[part], wo_v[2 * pos + 1])

    def chip_sum(part, off, u):
        pos = offsets.index(off)
        if (part, off) not in arrived:
            pair_copies[part, off].wait_recv()
            arrived.add((part, off))
        return part_v[part, pos, halves[u], :] + pair_recv[part, pos, halves[u], :].astype(F32)

    def hops(part, d):
        return far if part == d else far - 1

    def reduce_stage(part, stage):
        for u in (0, 1):
            for d in (0, 1):
                k = hops(part, d) - stage
                if k < 1:
                    continue
                value = chip_sum(part, (sign[d] * k) % chips, u)
                if stage:
                    rs_copies[part, d, stage - 1, u].wait_recv()
                    value = value + rs_recv[part, d, stage - 1, halves[u], :].astype(F32)
                rs_send[part, d, stage, halves[u], :] = value.astype(BF16)
                copy = pltpu.make_async_remote_copy(
                    src_ref=rs_send.at[part, d, stage, halves[u]], dst_ref=rs_recv.at[part, d, stage, halves[u]],
                    send_sem=rs_ssem.at[part, d, stage, u], recv_sem=rs_rsem.at[part, d, stage, u],
                    device_id=peer(nexts[d]), device_id_type=MESH)
                copy.start()
                rs_copies[part, d, stage, u] = copy

    def gather_send(part, d, stage, index, u):
        at = y_v.at[part, index, halves[u]]
        copy = pltpu.make_async_remote_copy(
            src_ref=at, dst_ref=at, send_sem=ag_ssem.at[part, d, stage, u], recv_sem=ag_rsem.at[part, d, stage, u],
            device_id=peer(nexts[d]), device_id_type=MESH)
        copy.start()
        ag_copies[part, d, stage, u] = copy

    def place_out(part, index, sem):
        out = pltpu.make_async_copy(
            y_v.at[part, index], y_hbm.at[pl.ds(part * total, total), block_at(index)], sem)
        out.start()
        out_copies.append(out)

    def spread(part, index, hop):
        at = y_v.at[part, index]
        copy = pltpu.make_async_remote_copy(
            src_ref=at, dst_ref=at, send_sem=d2d_ssem.at[part, hop], recv_sem=d2d_rsem.at[part, hop],
            device_id=peer(mate), device_id_type=MESH)
        copy.start()
        d2d_copies.append((copy, part, index + 1 - 2 * core, hop))
        place_out(part, index, out_sem.at[0, part, hop])

    def own_stage(part):
        for u in (0, 1):
            value = rest_v[part, halves[u], :] + chip_sum(part, 0, u)
            for d in (0, 1):
                stage = hops(part, d) - 1
                rs_copies[part, d, stage, u].wait_recv()
                value = value + rs_recv[part, d, stage, halves[u], :].astype(F32)
            y_v[part, own, halves[u], :] = value.astype(BF16)
            for d in (0, 1):
                gather_send(part, d, 0, own, u)
        spread(part, own, 0)

    def gather_stage(part, stage):
        for u in (0, 1):
            for d in (0, 1):
                if stage >= hops(part, d):
                    continue
                hop = (-sign[d] * (stage + 1)) % chips
                index = 2 * lax.rem(chip + hop, chips) + core
                ag_copies[part, d, stage, u].wait_recv()
                if stage + 1 < hops(part, d):
                    gather_send(part, d, stage + 1, index, u)
                if u == 1:
                    spread(part, index, hop)

    def stage_of(part, s):
        if s < far:
            reduce_stage(part, s)
        elif s == far:
            own_stage(part)
        elif s <= 2 * far:
            gather_stage(part, s - far - 1)

    for part in range(PARTS):
        collect(part)
        first = [far] + [(sign[1 - part] * (far - 1)) % chips]
        for off in first:
            multiply(part, off)
        for off in list(todo[part])[:2]:
            multiply(part, off)
        reduce_stage(part, 0)
        for off in list(todo[part]):
            multiply(part, off)
    for s in range(1, 2 * far + 2):
        for part in range(PARTS):
            if s > part:
                stage_of(part, s - part)
    for copy, part, other, hop in d2d_copies:
        copy.wait_recv()
        place_out(part, other, out_sem.at[1, part, hop])
    for copies in q_copies + o_copies:
        for copy in copies:
            copy.wait_send()
    for copy in list(pair_copies.values()) + list(rs_copies.values()) + list(ag_copies.values()):
        copy.wait_send()
    for copy, _, _, _ in d2d_copies:
        copy.wait_send()
    for out in out_copies:
        out.wait()


def order_kernel(n, local, y_ref, out_ref, hot_v):
    steps, group, cols = out_ref.shape
    total = steps * group
    share = local // PARTS

    @pl.when(pl.program_id(0) == 0)
    def _():
        row = iota((total, 1), 0)
        step, seq = row // group, row % group
        dev, i = seq // local, seq % local
        index = (i // share) * (total // PARTS) + step * (n * share) + dev * share + i % share
        hot_v[...] = one_hot(total, total, index)

    out_ref[...] = mm(hot_v[...], y_ref[...]).astype(BF16).reshape(steps, group, cols)


def solution(mesh):
    n = mesh.shape['tp']
    vmem = pl.BlockSpec(memory_space=pltpu.VMEM)
    smem = pl.BlockSpec(memory_space=pltpu.SMEM)
    anywhere = pl.BlockSpec(memory_space=pl.ANY)
    dma = pltpu.SemaphoreType.DMA

    def by_lanes(vector):
        return vector.reshape(-1, LANES)

    def local_block(x_steps, seq_lens, k_cache, v_cache, ln_gain, ln_bias, w_q, b_q, w_kv, b_kv, w_out, b_out):
        steps, group, width = x_steps.shape
        local, cache_len, head_dim = k_cache.shape
        total = steps * group
        q_cols = w_q.shape[1]
        kv_cols = w_kv.shape[1]
        heads = q_cols // head_dim
        per_seq = n * steps
        share = local // PARTS
        piece_cols = -(-share * steps * heads // PACK) * LANES
        piece_shape = (PARTS, n * PACK, piece_cols)
        pieces, k_out, v_out = pl.pallas_call(
            functools.partial(local_kernel, n),
            name='local',
            out_shape=(
                jax.ShapeDtypeStruct(piece_shape, BF16),
                jax.ShapeDtypeStruct(k_cache.shape, BF16),
                jax.ShapeDtypeStruct(v_cache.shape, BF16),
            ),
            in_specs=[smem, anywhere, vmem, vmem, anywhere, vmem, anywhere, vmem, anywhere, anywhere],
            out_specs=(vmem, anywhere, anywhere),
            scratch_shapes=[
                pltpu.VMEM((steps, group, width), BF16),
                pltpu.VMEM((total, width), BF16),
                pltpu.VMEM((width, q_cols), BF16),
                pltpu.VMEM((width, kv_cols), BF16),
                pltpu.VMEM(k_cache.shape, BF16),
                pltpu.VMEM(v_cache.shape, BF16),
                pltpu.VMEM((total, q_cols), F32),
                pltpu.VMEM((total, kv_cols), F32),
                pltpu.VMEM((1, width), F32),
                pltpu.VMEM((1, width), F32),
                pltpu.VMEM((1, q_cols), F32),
                pltpu.VMEM((1, kv_cols), F32),
                pltpu.VMEM((local * 8, kv_cols), F32),
                dma((steps,)), dma((2,)), dma((2, local)), dma((2, local)),
            ],
            compiler_params=pltpu.CompilerParams(vmem_limit_bytes=VMEM_LIMIT),
        )(seq_lens, x_steps, by_lanes(ln_gain), by_lanes(ln_bias), w_q, by_lanes(b_q), w_kv, by_lanes(b_kv), k_cache, v_cache)

        block = cache_len // 3 if cache_len % (3 * LANES) == 0 else cache_len
        cols = width // n
        chips = n // 2
        far = chips // 2
        rows = total // PARTS
        y = pl.pallas_call(
            functools.partial(group_kernel, n, steps, block),
            name='group',
            out_shape=jax.ShapeDtypeStruct((total, width), BF16),
            in_specs=[smem, anywhere, anywhere, anywhere, anywhere, anywhere, vmem],
            out_specs=anywhere,
            scratch_shapes=[
                pltpu.VMEM(piece_shape, BF16),
                pltpu.VMEM(piece_shape, BF16),
                pltpu.VMEM((share, heads * per_seq, head_dim), BF16),
                pltpu.VMEM(k_cache.shape, BF16),
                pltpu.VMEM(v_cache.shape, BF16),
                pltpu.VMEM((heads * per_seq, cache_len), F32),
                pltpu.VMEM((rows, q_cols), BF16),
                pltpu.VMEM(piece_shape, BF16),
                pltpu.VMEM(piece_shape, BF16),
                pltpu.VMEM((PARTS, rows, q_cols), BF16),
                pltpu.VMEM((n, q_cols, cols), BF16),
                pltpu.VMEM((total, cols), BF16),
                pltpu.VMEM((PARTS, rows, cols), F32),
                pltpu.VMEM((width // LANES, LANES), F32),
                pltpu.VMEM((PARTS, chips, rows, cols), F32),
                pltpu.VMEM((PARTS, chips, rows, cols), BF16),
                pltpu.VMEM((PARTS, chips, rows, cols), BF16),
                pltpu.VMEM((PARTS, 2, far, rows, cols), BF16),
                pltpu.VMEM((PARTS, 2, far, rows, cols), BF16),
                pltpu.VMEM((PARTS, n, rows, cols), BF16),
                dma((2,)), dma((local,)), dma((local,)), dma((n,)),
                dma((PARTS, n)), dma((PARTS, n)), dma((PARTS, n)), dma((PARTS, n)),
                dma((PARTS, chips)), dma((PARTS, chips)),
                dma((PARTS, 2, far, 2)), dma((PARTS, 2, far, 2)), dma((PARTS, 2, far, 2)), dma((PARTS, 2, far, 2)),
                dma((PARTS, chips)), dma((PARTS, chips)), dma((2, PARTS, chips)),
            ],
            compiler_params=pltpu.CompilerParams(
                collective_id=0, has_side_effects=True, vmem_limit_bytes=VMEM_LIMIT),
        )(seq_lens, pieces, k_out, v_out, x_steps.reshape(total, width), w_out, by_lanes(b_out))

        wide = 2 * cols
        y_steps = pl.pallas_call(
            functools.partial(order_kernel, n, local),
            name='order',
            grid=(width // wide,),
            out_shape=jax.ShapeDtypeStruct(x_steps.shape, BF16),
            in_specs=[pl.BlockSpec((total, wide), lambda c: (0, c))],
            out_specs=pl.BlockSpec((steps, group, wide), lambda c: (0, 0, c)),
            scratch_shapes=[pltpu.VMEM((total, total), BF16)],
        )(y)
        return y_steps, k_out, v_out

    row_spec = P(('dp', 'tp'), None, None)
    return jax.shard_map(
        local_block,
        mesh=mesh,
        in_specs=(P(None, 'dp', None), P(('dp', 'tp')), row_spec, row_spec, P(None), P(None), P(None, 'tp'), P('tp'), P(None, None), P(None), P('tp', None), P(None)),
        out_specs=(P(None, 'dp', None), row_spec, row_spec),
        check_vma=False,
    )
```

```python
import functools

import jax
import jax.numpy as jnp
from jax import lax
from jax.experimental import pallas as pl
from jax.experimental.pallas import tpu as pltpu
from jax.sharding import PartitionSpec as P

LN_EPS = 1e-5
LANES = 128
PACK = 16
PARTS = 2
VMEM_LIMIT = 60 * 1024 * 1024
GROUP_LIMIT = 44 * 1024 * 1024
ORDER_LIMIT = 16 * 1024 * 1024
MESH = pl.DeviceIdType.MESH
F32 = jnp.float32
BF16 = jnp.bfloat16


def iota(shape, dim):
    return lax.broadcasted_iota(jnp.int32, shape, dim)


def one_hot(rows, cols, index, valid=None):
    at = index if valid is None else jnp.where(valid, index, -1)
    return jnp.where(iota((rows, cols), 1) == at, 1.0, 0.0).astype(BF16)


def mm(a, b):
    return jnp.dot(a, b, preferred_element_type=F32)


def peer(index):
    return {'tp': index}


def tiles_of(head, rows):
    return range(head * rows // PACK, ((head + 1) * rows - 1) // PACK + 1)


def pairs_of(heads, rows):
    return [(tile, head) for head in range(heads) for tile in tiles_of(head, rows)]


def pack_hots(total, heads, source_row, n, rows):
    p = iota((n * PACK, 1), 0)
    dest, slot = p // PACK, p % PACK
    for tile, head in pairs_of(heads, rows):
        unit = tile * PACK + slot
        yield one_hot(n * PACK, total, source_row(dest, unit % rows), unit // rows == head)


def pack_rows(src, hots, heads, rows, send_buf):
    value = {}
    for (tile, head), hot in zip(pairs_of(heads, rows), hots):
        value[tile] = value.get(tile, 0.0) + mm(hot, src[:, head * LANES:(head + 1) * LANES])
    for tile in value:
        send_buf[:, tile * LANES:(tile + 1) * LANES] = value[tile].astype(BF16)


def unpack_hots(n, total, heads, place, rows):
    source, row = place(iota((total, 1), 0))
    for tile, head in pairs_of(heads, rows):
        unit = head * rows + row
        yield one_hot(total, n * PACK, source * PACK + unit % PACK, unit // PACK == tile)


def unpack_rows(recv_buf, hots, heads, rows):
    value = {}
    for (tile, head), hot in zip(pairs_of(heads, rows), hots):
        value[head] = value.get(head, 0.0) + mm(hot, recv_buf[:, tile * LANES:(tile + 1) * LANES])
    return [value[head].astype(BF16) for head in range(heads)]


def spread_row(row_ref, src_ref):
    for j in range(src_ref.shape[0]):
        row_ref[:, j * LANES:(j + 1) * LANES] = src_ref[j:j + 1, :].astype(F32)


def local_kernel(n, lens_ref, x_hbm, gain_ref, bias_ref, wq_hbm, bq_ref, wkv_hbm, bkv_ref, k_hbm, v_hbm,
                 pieces_ref, ko_hbm, vo_hbm,
                 x_v, h_v, wq_v, wkv_v, k_v, v_v, acc, kv_acc, gain_v, bias_v, bq_v, bkv_v, fresh,
                 x_sem, w_sem, in_sem, out_sem):
    me = lax.axis_index('tp')
    steps, group, width = x_v.shape
    q_cols = wq_v.shape[1]
    total = steps * group
    local, cache_len, head_dim = k_v.shape
    x_copies = [pltpu.make_async_copy(x_hbm.at[s], x_v.at[s], x_sem.at[s]) for s in range(steps)]
    wkv_copy = pltpu.make_async_copy(wkv_hbm, wkv_v, w_sem.at[0])
    wq_copy = pltpu.make_async_copy(wq_hbm, wq_v, w_sem.at[1])
    caches = ((k_hbm, k_v, ko_hbm), (v_hbm, v_v, vo_hbm))
    ins = [[pltpu.make_async_copy(src.at[i], mid.at[i], in_sem.at[c, i]) for i in range(local)]
           for c, (src, mid, _) in enumerate(caches)]
    outs = [[pltpu.make_async_copy(mid.at[i], dst.at[i], out_sem.at[c, i]) for i in range(local)]
            for c, (_, mid, dst) in enumerate(caches)]
    for copy in x_copies + [wkv_copy, wq_copy]:
        copy.start()
    for copy in ins[0] + ins[1]:
        copy.start(priority=1)
    spread_row(gain_v, gain_ref)
    spread_row(bias_v, bias_ref)
    spread_row(bq_v, bq_ref)
    spread_row(bkv_v, bkv_ref)

    for s in range(steps):
        x_copies[s].wait()

        @pl.loop(0, group // PACK)
        def _(r):
            at = pl.ds(pl.multiple_of(r * PACK, PACK), PACK)
            x = x_v[s, at, :].astype(F32)
            mean = jnp.mean(x, axis=-1, keepdims=True)
            centered = x - mean
            var = jnp.mean(centered * centered, axis=-1, keepdims=True)
            scaled = centered * lax.rsqrt(var + LN_EPS)
            h = (scaled * gain_v[...] + bias_v[...]).astype(BF16)
            h_v[pl.ds(pl.multiple_of(s * group + r * PACK, PACK), PACK), :] = h

    depth = width // 8

    def product(total_ref, w_v):
        total_ref[...] = jnp.zeros_like(total_ref)

        @pl.loop(0, width // depth)
        def _(c):
            at = pl.ds(pl.multiple_of(c * depth, depth), depth)
            total_ref[...] += mm(h_v[:, at], w_v[at, :])

    wkv_copy.wait()
    product(kv_acc, wkv_v)
    kv = (kv_acc[...] + bkv_v[...]).astype(BF16)
    pad = fresh.shape[0] // local
    row = iota((local * pad, 1), 0)
    fresh[...] = mm(one_hot(local * pad, total, (row % pad) * group + me * local + row // pad, row % pad < steps), kv)
    window = 2 * PACK
    for c in (0, 1):
        for i in range(local):
            mid = caches[c][1]
            seq_len = lens_ref[i]
            start = jnp.minimum((seq_len // PACK) * PACK, cache_len - window)
            at = pl.ds(pl.multiple_of(start, PACK), window)
            pos = iota((window, head_dim), 0) + start
            ins[c][i].wait()
            value = mid[i, at, :].astype(F32)
            for s in range(steps):
                new = fresh[i * pad + s:i * pad + s + 1, c * head_dim:(c + 1) * head_dim]
                value = jnp.where(pos == seq_len + s, new, value)
            mid[i, at, :] = value.astype(BF16)
            outs[c][i].start(priority=1)

    wq_copy.wait()
    product(acc, wq_v)
    q = (acc[...] + bq_v[...]).astype(BF16)
    share = local // PARTS
    for part in range(PARTS):
        hots = pack_hots(
            total, q_cols // LANES,
            lambda dest, r: (r % steps) * group + dest * local + part * share + r // steps, n, share * steps)
        pack_rows(q, hots, q_cols // LANES, share * steps, pieces_ref.at[part])
    for c in (0, 1):
        for copy in outs[c]:
            copy.wait()


def group_kernel(n, steps, block, lens_ref, pieces_hbm, k_hbm, v_hbm, x_hbm, wo_hbm, bo_ref, y_hbm,
                 pieces_v, q_recv, q_v, k_v, v_v, scores, heads_v, o_send, o_recv, a_v, wo_v, x_v, rest_v, bo_v,
                 part_v, pair_send, pair_recv, rs_send, rs_recv, y_v, pack_v, q_hot, o_hot,
                 in_sem, k_sem, v_sem, wo_sem, q_ssem, q_rsem, o_ssem, o_rsem, pair_ssem, pair_rsem,
                 rs_ssem, rs_rsem, ag_ssem, ag_rsem, d2d_ssem, d2d_rsem, out_sem):
    me = lax.axis_index('tp')
    local, cache_len, head_dim = k_v.shape
    share = local // PARTS
    rows = share * steps
    per_seq = n * steps
    total = share * per_seq
    depth = a_v.shape[2]
    heads = depth // head_dim
    cols = wo_v.shape[2]
    chips = n // 2
    far = chips // 2
    chip = me // 2
    core = me % 2
    mate = me + 1 - 2 * core
    group = local * n

    barrier = pltpu.get_barrier_semaphore()
    for k in range(1, n):
        pl.semaphore_signal(barrier, inc=1, device_id=peer(lax.rem(me + k, n)), device_id_type=MESH)

    def block_at(index):
        return pl.ds(pl.multiple_of(index * cols, LANES), cols)

    pieces_copy = pltpu.make_async_copy(pieces_hbm, pieces_v, in_sem.at[0])
    pieces_copy.start()
    x_copy = pltpu.make_async_copy(x_hbm.at[:, block_at(me)], x_v, in_sem.at[1])
    x_copy.start()

    cache_in = [(pltpu.make_async_copy(k_hbm.at[i], k_v.at[i], k_sem.at[i]),
                 pltpu.make_async_copy(v_hbm.at[i], v_v.at[i], v_sem.at[i])) for i in range(local)]
    for k_copy, v_copy in cache_in:
        k_copy.start()
        v_copy.start()
    offsets = [far]
    for k in range(far - 1, 0, -1):
        offsets += [k, chips - k]
    offsets.append(0)
    wo_copies = []
    for pos, off in enumerate(offsets):
        dest = lax.rem(chip + off, chips)
        for side, dev in enumerate((2 * dest + 1 - core, 2 * dest + core)):
            copy = pltpu.make_async_copy(wo_hbm.at[:, block_at(dev)], wo_v.at[2 * pos + side], wo_sem.at[2 * pos + side])
            copy.start()
            wo_copies.append(copy)

    bo_v[...] = bo_ref[...].astype(F32)
    tiles = cols // LANES
    bias = jnp.concatenate([bo_v[pl.ds(me * tiles + j, 1), :] for j in range(tiles)], axis=1)
    x_copy.wait()
    row = iota((total, 1), 0)
    for part in range(PARTS):
        source = (row // (n * share)) * group + ((row // share) % n) * local + part * share + row % share
        rest_v[part] = mm(one_hot(total, steps * group, source), x_v[...]) + bias

    def fill(ref, hots):
        for j, hot in enumerate(hots):
            ref[j] = hot

    def held(ref):
        return [ref[j] for j in range(ref.shape[0])]

    fill(q_hot, unpack_hots(
        n, total, heads, lambda row: ((row % per_seq) // steps, (row // per_seq) * steps + row % steps), rows))
    fill(pack_v, pack_hots(
        total, heads, lambda dest, r: (r // steps) * per_seq + dest * steps + r % steps, n, rows))
    fill(o_hot, unpack_hots(
        n, total, heads, lambda row: ((row // share) % n, (row % share) * steps + row // (n * share)), rows))

    def exchange(part, send_buf, recv_buf, send_sem, recv_sem):
        mine = pl.ds(pl.multiple_of(me * PACK, PACK), PACK)
        copies = []
        for k in sorted(range(1, n), key=lambda k: -min(k, n - k)):
            dest = lax.rem(me + k, n)
            copy = pltpu.make_async_remote_copy(
                src_ref=send_buf.at[part, pl.ds(pl.multiple_of(dest * PACK, PACK), PACK)],
                dst_ref=recv_buf.at[part, mine],
                send_sem=send_sem.at[part, k], recv_sem=recv_sem.at[part, k],
                device_id=peer(dest), device_id_type=MESH)
            copy.start()
            copies.append(copy)
        recv_buf[part, mine] = send_buf[part, mine]
        return copies

    pieces_copy.wait()
    pl.semaphore_wait(barrier, n - 1)
    q_copies = [exchange(part, pieces_v, q_recv, q_ssem, q_rsem) for part in range(PARTS)]

    n_rows = heads * per_seq
    factor = head_dim ** -0.5 * 1.4426950408889634
    col_step = iota((n_rows, block), 1) - iota((n_rows, block), 0) % steps

    def fold(value, op):
        out = value[:, :LANES]
        for c in range(1, block // LANES):
            out = op(out, value[:, c * LANES:(c + 1) * LANES])
        return out

    def attend(part):
        for copy in q_copies[part]:
            copy.wait_recv()
        by_head = unpack_rows(q_recv.at[part], held(q_hot), heads, rows)
        for i in range(share):
            for head in range(heads):
                q_v[i, head * per_seq:(head + 1) * per_seq, :] = by_head[head][i * per_seq:(i + 1) * per_seq]

        for copy in cache_in[part * share:(part + 1) * share]:
            copy[0].wait()
            copy[1].wait()

        @pl.loop(0, share)
        def _(i):
            seq = part * share + i
            seq_len = lens_ref[seq]
            q = q_v[i]
            top = jnp.full((n_rows, LANES), -jnp.inf, F32)
            for j in range(cache_len // block):
                at = slice(j * block, (j + 1) * block)
                t = lax.dot_general(q, k_v[seq, at, :], (((1,), (1,)), ((), ())), preferred_element_type=F32)
                t = jnp.where(col_step <= seq_len - j * block, t, -jnp.inf)
                scores[:, at] = t
                top = jnp.maximum(top, fold(t, jnp.maximum))
            top = jnp.max(top, axis=-1, keepdims=True)
            den = jnp.zeros((n_rows, LANES), F32)
            num = jnp.zeros((n_rows, head_dim), F32)
            for j in range(cache_len // block):
                at = slice(j * block, (j + 1) * block)
                p = jnp.exp2((scores[:, at] - top) * factor)
                num = num + mm(p.astype(BF16), v_v[seq, at, :])
                den = den + fold(p, jnp.add)
            out = (num / jnp.sum(den, axis=-1, keepdims=True)).astype(BF16)
            to = pl.ds(pl.multiple_of(i * per_seq, PACK), per_seq)
            for head in range(heads):
                heads_v[to, head * LANES:(head + 1) * LANES] = out[head * per_seq:(head + 1) * per_seq]

        pack_rows(heads_v[...], held(pack_v), heads, rows, o_send.at[part])
        return exchange(part, o_send, o_recv, o_ssem, o_rsem)

    o_copies = [attend(part) for part in range(PARTS)]

    cut = (total // 2 + PACK - 1) // PACK * PACK
    halves = (pl.ds(0, cut), pl.ds(cut, total - cut))
    sign = (-1, 1)
    nexts = [2 * lax.rem(chip + chips + sign[d], chips) + core for d in (0, 1)]
    own = 2 * chip + core
    pair_copies = {}
    arrived = set()
    loaded = set()
    rs_copies = {}
    ag_copies = {}
    d2d_copies = []
    out_copies = []
    todo = {part: list(offsets) for part in range(PARTS)}

    def collect(part):
        for copy in o_copies[part]:
            copy.wait_recv()
        by_head = unpack_rows(o_recv.at[part], held(o_hot), heads, rows)
        for head in range(heads):
            a_v[part, :, head * LANES:(head + 1) * LANES] = by_head[head]

    def multiply(part, off):
        todo[part].remove(off)
        pos = offsets.index(off)
        first = off not in loaded
        loaded.add(off)
        if first:
            wo_copies[2 * pos].wait()
        pair_send[part, pos] = mm(a_v[part], wo_v[2 * pos]).astype(BF16)
        copy = pltpu.make_async_remote_copy(
            src_ref=pair_send.at[part, pos], dst_ref=pair_recv.at[part, pos], send_sem=pair_ssem.at[part, pos],
            recv_sem=pair_rsem.at[part, pos], device_id=peer(mate), device_id_type=MESH)
        copy.start()
        pair_copies[part, off] = copy
        if first:
            wo_copies[2 * pos + 1].wait()
        part_v[part, pos] = mm(a_v[part], wo_v[2 * pos + 1])

    def chip_sum(part, off, u):
        pos = offsets.index(off)
        if (part, off) not in arrived:
            pair_copies[part, off].wait_recv()
            arrived.add((part, off))
        return part_v[part, pos, halves[u], :] + pair_recv[part, pos, halves[u], :].astype(F32)

    def hops(part, d):
        return far if part == d else far - 1

    def reduce_stage(part, stage):
        for u in (0, 1):
            for d in (0, 1):
                k = hops(part, d) - stage
                if k < 1:
                    continue
                value = chip_sum(part, (sign[d] * k) % chips, u)
                if stage:
                    rs_copies[part, d, stage - 1, u].wait_recv()
                    value = value + rs_recv[part, d, stage - 1, halves[u], :].astype(F32)
                rs_send[part, d, stage, halves[u], :] = value.astype(BF16)
                copy = pltpu.make_async_remote_copy(
                    src_ref=rs_send.at[part, d, stage, halves[u]], dst_ref=rs_recv.at[part, d, stage, halves[u]],
                    send_sem=rs_ssem.at[part, d, stage, u], recv_sem=rs_rsem.at[part, d, stage, u],
                    device_id=peer(nexts[d]), device_id_type=MESH)
                copy.start()
                rs_copies[part, d, stage, u] = copy

    def gather_send(part, d, stage, index, u):
        at = y_v.at[part, index, halves[u]]
        copy = pltpu.make_async_remote_copy(
            src_ref=at, dst_ref=at, send_sem=ag_ssem.at[part, d, stage, u], recv_sem=ag_rsem.at[part, d, stage, u],
            device_id=peer(nexts[d]), device_id_type=MESH)
        copy.start()
        ag_copies[part, d, stage, u] = copy

    def place_out(part, index, sem):
        out = pltpu.make_async_copy(
            y_v.at[part, index], y_hbm.at[pl.ds(part * total, total), block_at(index)], sem)
        out.start()
        out_copies.append(out)

    def spread(part, index, hop):
        at = y_v.at[part, index]
        copy = pltpu.make_async_remote_copy(
            src_ref=at, dst_ref=at, send_sem=d2d_ssem.at[part, hop], recv_sem=d2d_rsem.at[part, hop],
            device_id=peer(mate), device_id_type=MESH)
        copy.start()
        d2d_copies.append((copy, part, index + 1 - 2 * core, hop))
        place_out(part, index, out_sem.at[0, part, hop])

    def own_stage(part):
        for u in (0, 1):
            value = rest_v[part, halves[u], :] + chip_sum(part, 0, u)
            for d in (0, 1):
                stage = hops(part, d) - 1
                rs_copies[part, d, stage, u].wait_recv()
                value = value + rs_recv[part, d, stage, halves[u], :].astype(F32)
            y_v[part, own, halves[u], :] = value.astype(BF16)
            for d in (0, 1):
                gather_send(part, d, 0, own, u)
        spread(part, own, 0)

    def gather_stage(part, stage):
        for u in (0, 1):
            for d in (0, 1):
                if stage >= hops(part, d):
                    continue
                hop = (-sign[d] * (stage + 1)) % chips
                index = 2 * lax.rem(chip + hop, chips) + core
                ag_copies[part, d, stage, u].wait_recv()
                if stage + 1 < hops(part, d):
                    gather_send(part, d, stage + 1, index, u)
                if u == 1:
                    spread(part, index, hop)

    def stage_of(part, s):
        if s < far:
            reduce_stage(part, s)
        elif s == far:
            own_stage(part)
        elif s <= 2 * far:
            gather_stage(part, s - far - 1)

    def prepare(part, stage):
        need = [(sign[d] * (hops(part, d) - stage)) % chips for d in (0, 1)] if stage < far - 1 else todo[part]
        for off in list(need):
            if off in todo[part]:
                multiply(part, off)

    for part in range(PARTS):
        collect(part)
        prepare(part, 0)
        prepare(part, 1)
        stage_of(part, 0)
    for s in range(1, 2 * far + 2):
        for part in range(PARTS):
            if s > part:
                stage_of(part, s - part)
                prepare(part, s - part + 1)
    for copy, part, other, hop in d2d_copies:
        copy.wait_recv()
        place_out(part, other, out_sem.at[1, part, hop])
    for copies in q_copies + o_copies:
        for copy in copies:
            copy.wait_send()
    for copy in list(pair_copies.values()) + list(rs_copies.values()) + list(ag_copies.values()):
        copy.wait_send()
    for copy, _, _, _ in d2d_copies:
        copy.wait_send()
    for out in out_copies:
        out.wait()


def order_kernel(n, y_ref, out_ref, hot_v):
    steps, group, _ = out_ref.shape
    local = group // n
    share = local // PARTS

    @pl.when(pl.program_id(0) == 0)
    def _():
        seq = iota((group, 1), 0)
        dev, i = seq // local, seq % local
        hot_v[...] = one_hot(group, group, (i // share) * (n * share) + dev * share + i % share)

    for s in range(steps):
        src = jnp.concatenate([y_ref[part, s] for part in range(PARTS)], axis=0)
        out_ref[s] = mm(hot_v[...], src).astype(BF16)


def solution(mesh):
    n = mesh.shape['tp']
    vmem = pl.BlockSpec(memory_space=pltpu.VMEM)
    smem = pl.BlockSpec(memory_space=pltpu.SMEM)
    anywhere = pl.BlockSpec(memory_space=pl.ANY)
    dma = pltpu.SemaphoreType.DMA

    def in_hbm(array):
        return pltpu.with_memory_space_constraint(array, pltpu.HBM)

    def by_lanes(vector):
        return vector.reshape(-1, LANES)

    def local_block(x_steps, seq_lens, k_cache, v_cache, ln_gain, ln_bias, w_q, b_q, w_kv, b_kv, w_out, b_out):
        steps, group, width = x_steps.shape
        local, cache_len, head_dim = k_cache.shape
        total = steps * group
        q_cols = w_q.shape[1]
        kv_cols = w_kv.shape[1]
        heads = q_cols // head_dim
        per_seq = n * steps
        share = local // PARTS
        piece_cols = -(-share * steps * heads // PACK) * LANES
        piece_shape = (PARTS, n * PACK, piece_cols)
        pieces, k_out, v_out = pl.pallas_call(
            functools.partial(local_kernel, n),
            name='local',
            out_shape=(
                jax.ShapeDtypeStruct(piece_shape, BF16),
                jax.ShapeDtypeStruct(k_cache.shape, BF16),
                jax.ShapeDtypeStruct(v_cache.shape, BF16),
            ),
            in_specs=[smem, anywhere, vmem, vmem, anywhere, vmem, anywhere, vmem, anywhere, anywhere],
            out_specs=(vmem, anywhere, anywhere),
            scratch_shapes=[
                pltpu.VMEM((steps, group, width), BF16),
                pltpu.VMEM((total, width), BF16),
                pltpu.VMEM((width, q_cols), BF16),
                pltpu.VMEM((width, kv_cols), BF16),
                pltpu.VMEM(k_cache.shape, BF16),
                pltpu.VMEM(v_cache.shape, BF16),
                pltpu.VMEM((total, q_cols), F32),
                pltpu.VMEM((total, kv_cols), F32),
                pltpu.VMEM((1, width), F32),
                pltpu.VMEM((1, width), F32),
                pltpu.VMEM((1, q_cols), F32),
                pltpu.VMEM((1, kv_cols), F32),
                pltpu.VMEM((local * 8, kv_cols), F32),
                dma((steps,)), dma((2,)), dma((2, local)), dma((2, local)),
            ],
            compiler_params=pltpu.CompilerParams(vmem_limit_bytes=VMEM_LIMIT),
        )(seq_lens, x_steps, by_lanes(ln_gain), by_lanes(ln_bias), w_q, by_lanes(b_q), w_kv, by_lanes(b_kv), k_cache, v_cache)

        block = cache_len // 3 if cache_len % (3 * LANES) == 0 else cache_len
        cols = width // n
        chips = n // 2
        far = chips // 2
        rows = total // PARTS
        n_pairs = len(pairs_of(heads, share * steps))
        y = pl.pallas_call(
            functools.partial(group_kernel, n, steps, block),
            name='group',
            out_shape=jax.ShapeDtypeStruct((total, width), BF16),
            in_specs=[smem, anywhere, anywhere, anywhere, anywhere, anywhere, vmem],
            out_specs=anywhere,
            scratch_shapes=[
                pltpu.VMEM(piece_shape, BF16),
                pltpu.VMEM(piece_shape, BF16),
                pltpu.VMEM((share, heads * per_seq, head_dim), BF16),
                pltpu.VMEM(k_cache.shape, BF16),
                pltpu.VMEM(v_cache.shape, BF16),
                pltpu.VMEM((heads * per_seq, cache_len), F32),
                pltpu.VMEM((rows, q_cols), BF16),
                pltpu.VMEM(piece_shape, BF16),
                pltpu.VMEM(piece_shape, BF16),
                pltpu.VMEM((PARTS, rows, q_cols), BF16),
                pltpu.VMEM((n, q_cols, cols), BF16),
                pltpu.VMEM((total, cols), BF16),
                pltpu.VMEM((PARTS, rows, cols), F32),
                pltpu.VMEM((width // LANES, LANES), F32),
                pltpu.VMEM((PARTS, chips, rows, cols), F32),
                pltpu.VMEM((PARTS, chips, rows, cols), BF16),
                pltpu.VMEM((PARTS, chips, rows, cols), BF16),
                pltpu.VMEM((PARTS, 2, far, rows, cols), BF16),
                pltpu.VMEM((PARTS, 2, far, rows, cols), BF16),
                pltpu.VMEM((PARTS, n, rows, cols), BF16),
                pltpu.VMEM((n_pairs, n * PACK, rows), BF16),
                pltpu.VMEM((n_pairs, rows, n * PACK), BF16),
                pltpu.VMEM((n_pairs, rows, n * PACK), BF16),
                dma((2,)), dma((local,)), dma((local,)), dma((n,)),
                dma((PARTS, n)), dma((PARTS, n)), dma((PARTS, n)), dma((PARTS, n)),
                dma((PARTS, chips)), dma((PARTS, chips)),
                dma((PARTS, 2, far, 2)), dma((PARTS, 2, far, 2)), dma((PARTS, 2, far, 2)), dma((PARTS, 2, far, 2)),
                dma((PARTS, chips)), dma((PARTS, chips)), dma((2, PARTS, chips)),
            ],
            compiler_params=pltpu.CompilerParams(
                collective_id=0, has_side_effects=True, vmem_limit_bytes=GROUP_LIMIT),
        )(seq_lens, in_hbm(pieces), in_hbm(k_out), in_hbm(v_out), in_hbm(x_steps.reshape(total, width)), in_hbm(w_out),
          by_lanes(b_out))

        wide = 2 * cols
        y_steps = pl.pallas_call(
            functools.partial(order_kernel, n),
            name='order',
            grid=(width // wide,),
            out_shape=jax.ShapeDtypeStruct(x_steps.shape, BF16),
            in_specs=[pl.BlockSpec((PARTS, steps, group // PARTS, wide), lambda c: (0, 0, 0, c))],
            out_specs=pl.BlockSpec((steps, group, wide), lambda c: (0, 0, c)),
            scratch_shapes=[pltpu.VMEM((group, group), BF16)],
            compiler_params=pltpu.CompilerParams(vmem_limit_bytes=ORDER_LIMIT),
        )(y.reshape(PARTS, steps, group // PARTS, width))
        return y_steps, k_out, v_out

    row_spec = P(('dp', 'tp'), None, None)
    return jax.shard_map(
        local_block,
        mesh=mesh,
        in_specs=(P(None, 'dp', None), P(('dp', 'tp')), row_spec, row_spec, P(None), P(None), P(None, 'tp'), P('tp'), P(None, None), P(None), P('tp', None), P(None)),
        out_specs=(P(None, 'dp', None), row_spec, row_spec),
        check_vma=False,
    )
```

```python
import functools

import jax
import jax.numpy as jnp
from jax import lax
from jax.experimental import pallas as pl
from jax.experimental.pallas import tpu as pltpu
from jax.sharding import PartitionSpec as P

LN_EPS = 1e-5
LANES = 128
PACK = 16
PARTS = 2
VMEM_LIMIT = 60 * 1024 * 1024
GROUP_LIMIT = 44 * 1024 * 1024
ORDER_LIMIT = 16 * 1024 * 1024
MESH = pl.DeviceIdType.MESH
F32 = jnp.float32
BF16 = jnp.bfloat16


def iota(shape, dim):
    return lax.broadcasted_iota(jnp.int32, shape, dim)


def one_hot(rows, cols, index, valid=None):
    at = index if valid is None else jnp.where(valid, index, -1)
    return jnp.where(iota((rows, cols), 1) == at, 1.0, 0.0).astype(BF16)


def mm(a, b):
    return jnp.dot(a, b, preferred_element_type=F32)


def peer(index):
    return {'tp': index}


def tiles_of(head, rows):
    return range(head * rows // PACK, ((head + 1) * rows - 1) // PACK + 1)


def pairs_of(heads, rows):
    return [(tile, head) for head in range(heads) for tile in tiles_of(head, rows)]


def pack_hots(total, heads, source_row, n, rows):
    p = iota((n * PACK, 1), 0)
    dest, slot = p // PACK, p % PACK
    for tile, head in pairs_of(heads, rows):
        unit = tile * PACK + slot
        yield one_hot(n * PACK, total, source_row(dest, unit % rows), unit // rows == head)


def pack_rows(src, hots, heads, rows, send_buf):
    value = {}
    for (tile, head), hot in zip(pairs_of(heads, rows), hots):
        value[tile] = value.get(tile, 0.0) + mm(hot, src[:, head * LANES:(head + 1) * LANES])
    for tile in value:
        send_buf[:, tile * LANES:(tile + 1) * LANES] = value[tile].astype(BF16)


def unpack_hots(n, total, heads, place, rows):
    source, row = place(iota((total, 1), 0))
    for tile, head in pairs_of(heads, rows):
        unit = head * rows + row
        yield one_hot(total, n * PACK, source * PACK + unit % PACK, unit // PACK == tile)


def unpack_rows(recv_buf, hots, heads, rows):
    value = {}
    for (tile, head), hot in zip(pairs_of(heads, rows), hots):
        value[head] = value.get(head, 0.0) + mm(hot, recv_buf[:, tile * LANES:(tile + 1) * LANES])
    return [value[head].astype(BF16) for head in range(heads)]


def cut_of(rows):
    return -(-rows // (2 * PACK)) * PACK


def spread_row(row_ref, src_ref):
    for j in range(src_ref.shape[0]):
        row_ref[:, j * LANES:(j + 1) * LANES] = src_ref[j:j + 1, :].astype(F32)


def local_kernel(n, lens_ref, x_hbm, gain_ref, bias_ref, wq_hbm, bq_ref, wkv_hbm, bkv_ref, k_hbm, v_hbm,
                 pieces_ref, ko_hbm, vo_hbm,
                 x_v, h_v, wq_v, wkv_v, k_v, v_v, acc, kv_acc, gain_v, bias_v, bq_v, bkv_v, fresh,
                 x_sem, w_sem, in_sem, out_sem):
    me = lax.axis_index('tp')
    steps, group, width = x_v.shape
    q_cols = wq_v.shape[1]
    total = steps * group
    local, cache_len, head_dim = k_v.shape
    x_copies = [pltpu.make_async_copy(x_hbm.at[s], x_v.at[s], x_sem.at[s]) for s in range(steps)]
    wkv_copy = pltpu.make_async_copy(wkv_hbm, wkv_v, w_sem.at[0])
    wq_copy = pltpu.make_async_copy(wq_hbm, wq_v, w_sem.at[1])
    caches = ((k_hbm, k_v, ko_hbm), (v_hbm, v_v, vo_hbm))
    ins = [[pltpu.make_async_copy(src.at[i], mid.at[i], in_sem.at[c, i]) for i in range(local)]
           for c, (src, mid, _) in enumerate(caches)]
    outs = [[pltpu.make_async_copy(mid.at[i], dst.at[i], out_sem.at[c, i]) for i in range(local)]
            for c, (_, mid, dst) in enumerate(caches)]
    for copy in x_copies + [wkv_copy, wq_copy]:
        copy.start()
    for copy in ins[0] + ins[1]:
        copy.start(priority=1)
    spread_row(gain_v, gain_ref)
    spread_row(bias_v, bias_ref)
    spread_row(bq_v, bq_ref)
    spread_row(bkv_v, bkv_ref)

    for s in range(steps):
        x_copies[s].wait()

        @pl.loop(0, group // PACK)
        def _(r):
            at = pl.ds(pl.multiple_of(r * PACK, PACK), PACK)
            x = x_v[s, at, :].astype(F32)
            mean = jnp.mean(x, axis=-1, keepdims=True)
            centered = x - mean
            var = jnp.mean(centered * centered, axis=-1, keepdims=True)
            scaled = centered * lax.rsqrt(var + LN_EPS)
            h = (scaled * gain_v[...] + bias_v[...]).astype(BF16)
            h_v[pl.ds(pl.multiple_of(s * group + r * PACK, PACK), PACK), :] = h

    depth = width // 8

    def product(total_ref, w_v):
        total_ref[...] = jnp.zeros_like(total_ref)

        @pl.loop(0, width // depth)
        def _(c):
            at = pl.ds(pl.multiple_of(c * depth, depth), depth)
            total_ref[...] += mm(h_v[:, at], w_v[at, :])

    wkv_copy.wait()
    product(kv_acc, wkv_v)
    kv = (kv_acc[...] + bkv_v[...]).astype(BF16)
    pad = fresh.shape[0] // local
    row = iota((local * pad, 1), 0)
    fresh[...] = mm(one_hot(local * pad, total, (row % pad) * group + me * local + row // pad, row % pad < steps), kv)
    window = 2 * PACK
    for c in (0, 1):
        for i in range(local):
            mid = caches[c][1]
            seq_len = lens_ref[i]
            start = jnp.minimum((seq_len // PACK) * PACK, cache_len - window)
            at = pl.ds(pl.multiple_of(start, PACK), window)
            pos = iota((window, head_dim), 0) + start
            ins[c][i].wait()
            value = mid[i, at, :].astype(F32)
            for s in range(steps):
                new = fresh[i * pad + s:i * pad + s + 1, c * head_dim:(c + 1) * head_dim]
                value = jnp.where(pos == seq_len + s, new, value)
            mid[i, at, :] = value.astype(BF16)
            outs[c][i].start(priority=1)

    wq_copy.wait()
    product(acc, wq_v)
    q = (acc[...] + bq_v[...]).astype(BF16)
    share = local // PARTS
    for part in range(PARTS):
        hots = pack_hots(
            total, q_cols // LANES,
            lambda dest, r: (r % steps) * group + dest * local + part * share + r // steps, n, share * steps)
        pack_rows(q, hots, q_cols // LANES, share * steps, pieces_ref.at[part])
    for c in (0, 1):
        for copy in outs[c]:
            copy.wait()


def group_kernel(n, steps, block, lens_ref, pieces_hbm, k_hbm, v_hbm, x_hbm, wo_hbm, bo_ref, y_hbm,
                 pieces_v, q_recv, q_v, k_v, v_v, scores, heads_v, o_send, o_recv, a_v, wo_v, x_v, rest_v, bo_v,
                 part_v, pair_send, pair_recv, rs_send, rs_recv, y_v, pack_v, q_hot, o_hot,
                 in_sem, k_sem, v_sem, wo_sem, q_ssem, q_rsem, o_ssem, o_rsem, pair_ssem, pair_rsem,
                 rs_ssem, rs_rsem, ag_ssem, ag_rsem, d2d_ssem, d2d_rsem, out_sem):
    me = lax.axis_index('tp')
    local, cache_len, head_dim = k_v.shape
    share = local // PARTS
    rows = share * steps
    per_seq = n * steps
    total = share * per_seq
    depth = a_v.shape[2]
    heads = depth // head_dim
    cols = wo_v.shape[2]
    chips = n // 2
    far = chips // 2
    chip = me // 2
    core = me % 2
    mate = me + 1 - 2 * core
    group = local * n

    barrier = pltpu.get_barrier_semaphore()
    for k in range(1, n):
        pl.semaphore_signal(barrier, inc=1, device_id=peer(lax.rem(me + k, n)), device_id_type=MESH)

    def block_at(index):
        return pl.ds(pl.multiple_of(index * cols, LANES), cols)

    pieces_copy = pltpu.make_async_copy(pieces_hbm, pieces_v, in_sem.at[0])
    pieces_copy.start()
    x_copy = pltpu.make_async_copy(x_hbm.at[:, block_at(me)], x_v, in_sem.at[1])
    x_copy.start()

    cache_in = [(pltpu.make_async_copy(k_hbm.at[i], k_v.at[i], k_sem.at[i]),
                 pltpu.make_async_copy(v_hbm.at[i], v_v.at[i], v_sem.at[i])) for i in range(local)]
    for k_copy, v_copy in cache_in:
        k_copy.start()
        v_copy.start()
    offsets = [far]
    for k in range(far - 1, 0, -1):
        offsets += [k, chips - k]
    offsets.append(0)
    wo_copies = []
    for pos, off in enumerate(offsets):
        dest = lax.rem(chip + off, chips)
        for side, dev in enumerate((2 * dest + 1 - core, 2 * dest + core)):
            copy = pltpu.make_async_copy(wo_hbm.at[:, block_at(dev)], wo_v.at[2 * pos + side], wo_sem.at[2 * pos + side])
            copy.start()
            wo_copies.append(copy)

    bo_v[...] = bo_ref[...].astype(F32)
    tiles = cols // LANES
    bias = jnp.concatenate([bo_v[pl.ds(me * tiles + j, 1), :] for j in range(tiles)], axis=1)
    x_copy.wait()
    row = iota((total, 1), 0)
    for part in range(PARTS):
        source = (row // (n * share)) * group + ((row // share) % n) * local + part * share + row % share
        rest_v[part] = mm(one_hot(total, steps * group, source), x_v[...]) + bias

    def fill(ref, hots):
        for j, hot in enumerate(hots):
            ref[j] = hot

    def held(ref):
        return [ref[j] for j in range(ref.shape[0])]

    fill(q_hot, unpack_hots(
        n, total, heads, lambda row: ((row % per_seq) // steps, (row // per_seq) * steps + row % steps), rows))
    fill(pack_v, pack_hots(
        total, heads, lambda dest, r: (r // steps) * per_seq + dest * steps + r % steps, n, rows))
    fill(o_hot, unpack_hots(
        n, total, heads, lambda row: ((row // share) % n, (row % share) * steps + row // (n * share)), rows))

    def exchange(part, send_buf, recv_buf, send_sem, recv_sem):
        mine = pl.ds(pl.multiple_of(me * PACK, PACK), PACK)
        copies = []
        for k in sorted(range(1, n), key=lambda k: -min(k, n - k)):
            dest = lax.rem(me + k, n)
            copy = pltpu.make_async_remote_copy(
                src_ref=send_buf.at[part, pl.ds(pl.multiple_of(dest * PACK, PACK), PACK)],
                dst_ref=recv_buf.at[part, mine],
                send_sem=send_sem.at[part, k], recv_sem=recv_sem.at[part, k],
                device_id=peer(dest), device_id_type=MESH)
            copy.start()
            copies.append(copy)
        recv_buf[part, mine] = send_buf[part, mine]
        return copies

    pieces_copy.wait()
    pl.semaphore_wait(barrier, n - 1)
    q_copies = [exchange(part, pieces_v, q_recv, q_ssem, q_rsem) for part in range(PARTS)]

    n_rows = heads * per_seq
    factor = head_dim ** -0.5 * 1.4426950408889634
    col_step = iota((n_rows, block), 1) - iota((n_rows, block), 0) % steps

    def fold(value, op):
        out = value[:, :LANES]
        for c in range(1, block // LANES):
            out = op(out, value[:, c * LANES:(c + 1) * LANES])
        return out

    def attend(part):
        for copy in q_copies[part]:
            copy.wait_recv()
        by_head = unpack_rows(q_recv.at[part], held(q_hot), heads, rows)
        for i in range(share):
            for head in range(heads):
                q_v[i, head * per_seq:(head + 1) * per_seq, :] = by_head[head][i * per_seq:(i + 1) * per_seq]

        for copy in cache_in[part * share:(part + 1) * share]:
            copy[0].wait()
            copy[1].wait()

        @pl.loop(0, share)
        def _(i):
            seq = part * share + i
            seq_len = lens_ref[seq]
            q = q_v[i]
            top = jnp.full((n_rows, LANES), -jnp.inf, F32)
            for j in range(cache_len // block):
                at = slice(j * block, (j + 1) * block)
                t = lax.dot_general(q, k_v[seq, at, :], (((1,), (1,)), ((), ())), preferred_element_type=F32)
                t = jnp.where(col_step <= seq_len - j * block, t, -jnp.inf)
                scores[:, at] = t
                top = jnp.maximum(top, fold(t, jnp.maximum))
            top = jnp.max(top, axis=-1, keepdims=True)
            den = jnp.zeros((n_rows, LANES), F32)
            num = jnp.zeros((n_rows, head_dim), F32)
            for j in range(cache_len // block):
                at = slice(j * block, (j + 1) * block)
                p = jnp.exp2((scores[:, at] - top) * factor)
                num = num + mm(p.astype(BF16), v_v[seq, at, :])
                den = den + fold(p, jnp.add)
            out = (num / jnp.sum(den, axis=-1, keepdims=True)).astype(BF16)
            to = pl.ds(pl.multiple_of(i * per_seq, PACK), per_seq)
            for head in range(heads):
                heads_v[to, head * LANES:(head + 1) * LANES] = out[head * per_seq:(head + 1) * per_seq]

        pack_rows(heads_v[...], held(pack_v), heads, rows, o_send.at[part])
        return exchange(part, o_send, o_recv, o_ssem, o_rsem)

    o_copies = [attend(part) for part in range(PARTS)]

    cut = cut_of(total)
    sizes = (cut, total - cut)
    halves = (pl.ds(0, cut), pl.ds(cut, total - cut))
    sign = (-1, 1)
    nexts = [2 * lax.rem(chip + chips + sign[d], chips) + core for d in (0, 1)]
    own = 2 * chip + core
    pair_copies = {}
    arrived = set()
    loaded = set()
    rs_copies = {}
    ag_copies = {}
    d2d_copies = []
    out_copies = []
    todo = {part: list(offsets) for part in range(PARTS)}

    def collect(part):
        for copy in o_copies[part]:
            copy.wait_recv()
        by_head = unpack_rows(o_recv.at[part], held(o_hot), heads, rows)
        for head in range(heads):
            a_v[part, :, head * LANES:(head + 1) * LANES] = by_head[head]

    def multiply(part, off):
        todo[part].remove(off)
        pos = offsets.index(off)
        first = off not in loaded
        loaded.add(off)
        if first:
            wo_copies[2 * pos].wait()
        pair_send[part, pos] = mm(a_v[part], wo_v[2 * pos]).astype(BF16)
        copy = pltpu.make_async_remote_copy(
            src_ref=pair_send.at[part, pos], dst_ref=pair_recv.at[part, pos], send_sem=pair_ssem.at[part, pos],
            recv_sem=pair_rsem.at[part, pos], device_id=peer(mate), device_id_type=MESH)
        copy.start()
        pair_copies[part, off] = copy
        if first:
            wo_copies[2 * pos + 1].wait()
        part_v[part, pos] = mm(a_v[part], wo_v[2 * pos + 1])

    def chip_sum(part, off, u):
        pos = offsets.index(off)
        if (part, off) not in arrived:
            pair_copies[part, off].wait_recv()
            arrived.add((part, off))
        return part_v[part, pos, halves[u], :] + pair_recv[part, pos, halves[u], :].astype(F32)

    def lone(part, d):
        return d ^ part

    plan = {
        (part, d): [(far, lone(part, d))] + [(k, h) for k in range(far - 1, 0, -1) for h in (1 - lone(part, d), lone(part, d))]
        for part in range(PARTS) for d in (0, 1)}
    n_slots = 2 * far - 1

    def reduce_slot(part, slot):
        for d in (0, 1):
            k, u = plan[part, d][slot]
            value = chip_sum(part, (sign[d] * k) % chips, u)
            if slot >= 2:
                rs_copies[part, d, slot - 2].wait_recv()
                value = value + rs_recv[part, d, slot - 2, :sizes[u], :].astype(F32)
            rs_send[part, d, slot, :sizes[u], :] = value.astype(BF16)
            copy = pltpu.make_async_remote_copy(
                src_ref=rs_send.at[part, d, slot, pl.ds(0, sizes[u])], dst_ref=rs_recv.at[part, d, slot, pl.ds(0, sizes[u])],
                send_sem=rs_ssem.at[part, d, slot], recv_sem=rs_rsem.at[part, d, slot],
                device_id=peer(nexts[d]), device_id_type=MESH)
            copy.start()
            rs_copies[part, d, slot] = copy

    def gather_send(part, d, slot, index, u):
        at = y_v.at[part, index, halves[u]]
        copy = pltpu.make_async_remote_copy(
            src_ref=at, dst_ref=at, send_sem=ag_ssem.at[part, d, slot], recv_sem=ag_rsem.at[part, d, slot],
            device_id=peer(nexts[d]), device_id_type=MESH)
        copy.start()
        ag_copies[part, d, slot] = copy

    def place_out(part, index, sem):
        out = pltpu.make_async_copy(
            y_v.at[part, index], y_hbm.at[pl.ds(part * total, total), block_at(index)], sem)
        out.start()
        out_copies.append(out)

    def spread(part, index, hop):
        at = y_v.at[part, index]
        copy = pltpu.make_async_remote_copy(
            src_ref=at, dst_ref=at, send_sem=d2d_ssem.at[part, hop], recv_sem=d2d_rsem.at[part, hop],
            device_id=peer(mate), device_id_type=MESH)
        copy.start()
        d2d_copies.append((copy, part, index + 1 - 2 * core, hop))
        place_out(part, index, out_sem.at[0, part, hop])

    def own_step(part):
        for u in (0, 1):
            value = rest_v[part, halves[u], :] + chip_sum(part, 0, u)
            for d in (0, 1):
                slot = n_slots - 1 if lone(part, d) == u else n_slots - 2
                rs_copies[part, d, slot].wait_recv()
                value = value + rs_recv[part, d, slot, :sizes[u], :].astype(F32)
            y_v[part, own, halves[u], :] = value.astype(BF16)
        for slot in (0, 1):
            for d in (0, 1):
                gather_send(part, d, slot, own, lone(part, d) if slot else 1 - lone(part, d))
        spread(part, own, 0)

    landed = {}

    def gather_slot(part, slot):
        for d in (0, 1):
            u = lone(part, d) if slot % 2 else 1 - lone(part, d)
            hop = (-sign[d] * (slot // 2 + 1)) % chips
            index = 2 * lax.rem(chip + hop, chips) + core
            ag_copies[part, d, slot].wait_recv()
            if slot + 2 < n_slots:
                gather_send(part, d, slot + 2, index, u)
            landed[part, hop] = landed.get((part, hop), 0) + 1
            if landed[part, hop] == 2:
                spread(part, index, hop)

    def prepare(part, slot):
        need = [(sign[d] * plan[part, d][slot][0]) % chips for d in (0, 1)] if slot < n_slots else todo[part]
        for off in list(need):
            if off in todo[part]:
                multiply(part, off)

    def step_of(part, s):
        if 0 <= s < n_slots:
            prepare(part, s + 2)
            reduce_slot(part, s)
        elif s == n_slots:
            own_step(part)
        elif n_slots < s <= 2 * n_slots:
            gather_slot(part, s - n_slots - 1)

    lag = 2
    for part in range(PARTS):
        collect(part)
        prepare(part, 0)
        prepare(part, 1)
        if part == 0:
            for s in range(lag):
                step_of(0, s)
    for s in range(lag, 2 * n_slots + 1 + lag):
        for part in range(PARTS):
            step_of(part, s - part * lag)
    for copy, part, other, hop in d2d_copies:
        copy.wait_recv()
        place_out(part, other, out_sem.at[1, part, hop])
    for copies in q_copies + o_copies:
        for copy in copies:
            copy.wait_send()
    for copy in list(pair_copies.values()) + list(rs_copies.values()) + list(ag_copies.values()):
        copy.wait_send()
    for copy, _, _, _ in d2d_copies:
        copy.wait_send()
    for out in out_copies:
        out.wait()


def order_kernel(n, y_ref, out_ref, hot_v):
    steps, group, _ = out_ref.shape
    local = group // n
    share = local // PARTS

    @pl.when(pl.program_id(0) == 0)
    def _():
        seq = iota((group, 1), 0)
        dev, i = seq // local, seq % local
        hot_v[...] = one_hot(group, group, (i // share) * (n * share) + dev * share + i % share)

    for s in range(steps):
        src = jnp.concatenate([y_ref[part, s] for part in range(PARTS)], axis=0)
        out_ref[s] = mm(hot_v[...], src).astype(BF16)


def solution(mesh):
    n = mesh.shape['tp']
    vmem = pl.BlockSpec(memory_space=pltpu.VMEM)
    smem = pl.BlockSpec(memory_space=pltpu.SMEM)
    anywhere = pl.BlockSpec(memory_space=pl.ANY)
    dma = pltpu.SemaphoreType.DMA

    def in_hbm(array):
        return pltpu.with_memory_space_constraint(array, pltpu.HBM)

    def by_lanes(vector):
        return vector.reshape(-1, LANES)

    def local_block(x_steps, seq_lens, k_cache, v_cache, ln_gain, ln_bias, w_q, b_q, w_kv, b_kv, w_out, b_out):
        steps, group, width = x_steps.shape
        local, cache_len, head_dim = k_cache.shape
        total = steps * group
        q_cols = w_q.shape[1]
        kv_cols = w_kv.shape[1]
        heads = q_cols // head_dim
        per_seq = n * steps
        share = local // PARTS
        piece_cols = -(-share * steps * heads // PACK) * LANES
        piece_shape = (PARTS, n * PACK, piece_cols)
        pieces, k_out, v_out = pl.pallas_call(
            functools.partial(local_kernel, n),
            name='local',
            out_shape=(
                jax.ShapeDtypeStruct(piece_shape, BF16),
                jax.ShapeDtypeStruct(k_cache.shape, BF16),
                jax.ShapeDtypeStruct(v_cache.shape, BF16),
            ),
            in_specs=[smem, anywhere, vmem, vmem, anywhere, vmem, anywhere, vmem, anywhere, anywhere],
            out_specs=(vmem, anywhere, anywhere),
            scratch_shapes=[
                pltpu.VMEM((steps, group, width), BF16),
                pltpu.VMEM((total, width), BF16),
                pltpu.VMEM((width, q_cols), BF16),
                pltpu.VMEM((width, kv_cols), BF16),
                pltpu.VMEM(k_cache.shape, BF16),
                pltpu.VMEM(v_cache.shape, BF16),
                pltpu.VMEM((total, q_cols), F32),
                pltpu.VMEM((total, kv_cols), F32),
                pltpu.VMEM((1, width), F32),
                pltpu.VMEM((1, width), F32),
                pltpu.VMEM((1, q_cols), F32),
                pltpu.VMEM((1, kv_cols), F32),
                pltpu.VMEM((local * 8, kv_cols), F32),
                dma((steps,)), dma((2,)), dma((2, local)), dma((2, local)),
            ],
            compiler_params=pltpu.CompilerParams(vmem_limit_bytes=VMEM_LIMIT),
        )(seq_lens, x_steps, by_lanes(ln_gain), by_lanes(ln_bias), w_q, by_lanes(b_q), w_kv, by_lanes(b_kv), k_cache, v_cache)

        block = cache_len // 3 if cache_len % (3 * LANES) == 0 else cache_len
        cols = width // n
        chips = n // 2
        far = chips // 2
        rows = total // PARTS
        n_pairs = len(pairs_of(heads, share * steps))
        cut = cut_of(rows)
        y = pl.pallas_call(
            functools.partial(group_kernel, n, steps, block),
            name='group',
            out_shape=jax.ShapeDtypeStruct((total, width), BF16),
            in_specs=[smem, anywhere, anywhere, anywhere, anywhere, anywhere, vmem],
            out_specs=anywhere,
            scratch_shapes=[
                pltpu.VMEM(piece_shape, BF16),
                pltpu.VMEM(piece_shape, BF16),
                pltpu.VMEM((share, heads * per_seq, head_dim), BF16),
                pltpu.VMEM(k_cache.shape, BF16),
                pltpu.VMEM(v_cache.shape, BF16),
                pltpu.VMEM((heads * per_seq, cache_len), F32),
                pltpu.VMEM((rows, q_cols), BF16),
                pltpu.VMEM(piece_shape, BF16),
                pltpu.VMEM(piece_shape, BF16),
                pltpu.VMEM((PARTS, rows, q_cols), BF16),
                pltpu.VMEM((n, q_cols, cols), BF16),
                pltpu.VMEM((total, cols), BF16),
                pltpu.VMEM((PARTS, rows, cols), F32),
                pltpu.VMEM((width // LANES, LANES), F32),
                pltpu.VMEM((PARTS, chips, rows, cols), F32),
                pltpu.VMEM((PARTS, chips, rows, cols), BF16),
                pltpu.VMEM((PARTS, chips, rows, cols), BF16),
                pltpu.VMEM((PARTS, 2, 2 * far - 1, cut, cols), BF16),
                pltpu.VMEM((PARTS, 2, 2 * far - 1, cut, cols), BF16),
                pltpu.VMEM((PARTS, n, rows, cols), BF16),
                pltpu.VMEM((n_pairs, n * PACK, rows), BF16),
                pltpu.VMEM((n_pairs, rows, n * PACK), BF16),
                pltpu.VMEM((n_pairs, rows, n * PACK), BF16),
                dma((2,)), dma((local,)), dma((local,)), dma((n,)),
                dma((PARTS, n)), dma((PARTS, n)), dma((PARTS, n)), dma((PARTS, n)),
                dma((PARTS, chips)), dma((PARTS, chips)),
                dma((PARTS, 2, 2 * far - 1)), dma((PARTS, 2, 2 * far - 1)),
                dma((PARTS, 2, 2 * far - 1)), dma((PARTS, 2, 2 * far - 1)),
                dma((PARTS, chips)), dma((PARTS, chips)), dma((2, PARTS, chips)),
            ],
            compiler_params=pltpu.CompilerParams(
                collective_id=0, has_side_effects=True, vmem_limit_bytes=GROUP_LIMIT),
        )(seq_lens, in_hbm(pieces), in_hbm(k_out), in_hbm(v_out), in_hbm(x_steps.reshape(total, width)), in_hbm(w_out),
          by_lanes(b_out))

        wide = 2 * cols
        y_steps = pl.pallas_call(
            functools.partial(order_kernel, n),
            name='order',
            grid=(width // wide,),
            out_shape=jax.ShapeDtypeStruct(x_steps.shape, BF16),
            in_specs=[pl.BlockSpec((PARTS, steps, group // PARTS, wide), lambda c: (0, 0, 0, c))],
            out_specs=pl.BlockSpec((steps, group, wide), lambda c: (0, 0, c)),
            scratch_shapes=[pltpu.VMEM((group, group), BF16)],
            compiler_params=pltpu.CompilerParams(vmem_limit_bytes=ORDER_LIMIT),
        )(y.reshape(PARTS, steps, group // PARTS, width))
        return y_steps, k_out, v_out

    row_spec = P(('dp', 'tp'), None, None)
    return jax.shard_map(
        local_block,
        mesh=mesh,
        in_specs=(P(None, 'dp', None), P(('dp', 'tp')), row_spec, row_spec, P(None), P(None), P(None, 'tp'), P('tp'), P(None, None), P(None), P('tp', None), P(None)),
        out_specs=(P(None, 'dp', None), row_spec, row_spec),
        check_vma=False,
    )
```

```python
import functools

import jax
import jax.numpy as jnp
from jax import lax
from jax.experimental import pallas as pl
from jax.experimental.pallas import tpu as pltpu
from jax.sharding import PartitionSpec as P

LN_EPS = 1e-5
LANES = 128
PACK = 16
PARTS = 2
VMEM_LIMIT = 60 * 1024 * 1024
GROUP_LIMIT = 44 * 1024 * 1024
ORDER_LIMIT = 16 * 1024 * 1024
MESH = pl.DeviceIdType.MESH
F32 = jnp.float32
BF16 = jnp.bfloat16


def iota(shape, dim):
    return lax.broadcasted_iota(jnp.int32, shape, dim)


def one_hot(rows, cols, index, valid=None):
    at = index if valid is None else jnp.where(valid, index, -1)
    return jnp.where(iota((rows, cols), 1) == at, 1.0, 0.0).astype(BF16)


def mm(a, b):
    return jnp.dot(a, b, preferred_element_type=F32)


def peer(index):
    return {'tp': index}


def tiles_of(head, rows):
    return range(head * rows // PACK, ((head + 1) * rows - 1) // PACK + 1)


def pairs_of(heads, rows):
    return [(tile, head) for head in range(heads) for tile in tiles_of(head, rows)]


def pack_hots(total, heads, source_row, n, rows):
    p = iota((n * PACK, 1), 0)
    dest, slot = p // PACK, p % PACK
    for tile, head in pairs_of(heads, rows):
        unit = tile * PACK + slot
        yield one_hot(n * PACK, total, source_row(dest, unit % rows), unit // rows == head)


def pack_rows(src, hots, heads, rows, send_buf):
    value = {}
    for (tile, head), hot in zip(pairs_of(heads, rows), hots):
        value[tile] = value.get(tile, 0.0) + mm(hot, src[:, head * LANES:(head + 1) * LANES])
    for tile in value:
        send_buf[:, tile * LANES:(tile + 1) * LANES] = value[tile].astype(BF16)


def unpack_hots(n, total, heads, place, rows):
    source, row = place(iota((total, 1), 0))
    for tile, head in pairs_of(heads, rows):
        unit = head * rows + row
        yield one_hot(total, n * PACK, source * PACK + unit % PACK, unit // PACK == tile)


def unpack_rows(recv_buf, hots, heads, rows):
    value = {}
    for (tile, head), hot in zip(pairs_of(heads, rows), hots):
        value[head] = value.get(head, 0.0) + mm(hot, recv_buf[:, tile * LANES:(tile + 1) * LANES])
    return [value[head].astype(BF16) for head in range(heads)]


def cut_of(rows):
    return -(-rows // (2 * PACK)) * PACK


def spread_row(row_ref, src_ref):
    for j in range(src_ref.shape[0]):
        row_ref[:, j * LANES:(j + 1) * LANES] = src_ref[j:j + 1, :].astype(F32)


def local_kernel(n, lens_hbm, x_hbm, gain_hbm, bias_hbm, wq_hbm, bq_hbm, wkv_hbm, bkv_hbm, k_hbm, v_hbm,
                 pieces_hbm, ko_hbm, vo_hbm,
                 x_v, h_v, wq_v, wkv_v, k_v, v_v, acc, kv_acc, gain_v, bias_v, bq_v, bkv_v, fresh,
                 pieces_v, gain_ref, bias_ref, bq_ref, bkv_ref, lens_ref,
                 x_sem, w_sem, in_sem, out_sem, small_sem, piece_sem):
    me = lax.axis_index('tp')
    steps, group, width = x_v.shape
    q_cols = wq_v.shape[1]
    total = steps * group
    local, cache_len, head_dim = k_v.shape
    x_copies = [pltpu.make_async_copy(x_hbm.at[s], x_v.at[s], x_sem.at[s]) for s in range(steps)]
    wkv_copy = pltpu.make_async_copy(wkv_hbm, wkv_v, w_sem.at[0])
    wq_copy = pltpu.make_async_copy(wq_hbm, wq_v, w_sem.at[1])
    caches = ((k_hbm, k_v, ko_hbm), (v_hbm, v_v, vo_hbm))
    ins = [[pltpu.make_async_copy(src.at[i], mid.at[i], in_sem.at[c, i]) for i in range(local)]
           for c, (src, mid, _) in enumerate(caches)]
    outs = [[pltpu.make_async_copy(mid.at[i], dst.at[i], out_sem.at[c, i]) for i in range(local)]
            for c, (_, mid, dst) in enumerate(caches)]
    small = [pltpu.make_async_copy(src, dst, small_sem.at[j]) for j, (src, dst) in enumerate((
        (gain_hbm, gain_ref), (bias_hbm, bias_ref), (bq_hbm, bq_ref), (bkv_hbm, bkv_ref), (lens_hbm, lens_ref)))]
    for copy in x_copies[:1] + small + x_copies[1:] + [wkv_copy, wq_copy]:
        copy.start()
    for copy in ins[0] + ins[1]:
        copy.start(priority=1)
    for copy in small:
        copy.wait()
    spread_row(gain_v, gain_ref)
    spread_row(bias_v, bias_ref)
    spread_row(bq_v, bq_ref)
    spread_row(bkv_v, bkv_ref)

    for s in range(steps):
        x_copies[s].wait()

        @pl.loop(0, group // PACK)
        def _(r):
            at = pl.ds(pl.multiple_of(r * PACK, PACK), PACK)
            x = x_v[s, at, :].astype(F32)
            mean = jnp.mean(x, axis=-1, keepdims=True)
            centered = x - mean
            var = jnp.mean(centered * centered, axis=-1, keepdims=True)
            scaled = centered * lax.rsqrt(var + LN_EPS)
            h = (scaled * gain_v[...] + bias_v[...]).astype(BF16)
            h_v[pl.ds(pl.multiple_of(s * group + r * PACK, PACK), PACK), :] = h

    depth = width // 8

    def product(total_ref, w_v):
        total_ref[...] = jnp.zeros_like(total_ref)

        @pl.loop(0, width // depth)
        def _(c):
            at = pl.ds(pl.multiple_of(c * depth, depth), depth)
            total_ref[...] += mm(h_v[:, at], w_v[at, :])

    wkv_copy.wait()
    product(kv_acc, wkv_v)
    kv = (kv_acc[...] + bkv_v[...]).astype(BF16)
    pad = fresh.shape[0] // local
    row = iota((local * pad, 1), 0)
    fresh[...] = mm(one_hot(local * pad, total, (row % pad) * group + me * local + row // pad, row % pad < steps), kv)
    window = 2 * PACK
    for c in (0, 1):
        for i in range(local):
            mid = caches[c][1]
            seq_len = lens_ref[i]
            start = jnp.minimum((seq_len // PACK) * PACK, cache_len - window)
            at = pl.ds(pl.multiple_of(start, PACK), window)
            pos = iota((window, head_dim), 0) + start
            ins[c][i].wait()
            value = mid[i, at, :].astype(F32)
            for s in range(steps):
                new = fresh[i * pad + s:i * pad + s + 1, c * head_dim:(c + 1) * head_dim]
                value = jnp.where(pos == seq_len + s, new, value)
            mid[i, at, :] = value.astype(BF16)
            outs[c][i].start(priority=1)

    wq_copy.wait()
    product(acc, wq_v)
    q = (acc[...] + bq_v[...]).astype(BF16)
    share = local // PARTS
    pieces = []
    for part in range(PARTS):
        hots = pack_hots(
            total, q_cols // LANES,
            lambda dest, r: (r % steps) * group + dest * local + part * share + r // steps, n, share * steps)
        pack_rows(q, hots, q_cols // LANES, share * steps, pieces_v.at[part])
        piece = pltpu.make_async_copy(pieces_v.at[part], pieces_hbm.at[part], piece_sem.at[part])
        piece.start()
        pieces.append(piece)
    for copy in outs[0] + outs[1] + pieces:
        copy.wait()


def group_kernel(n, steps, block, lens_hbm, pieces_hbm, k_hbm, v_hbm, x_hbm, wo_hbm, bo_hbm, y_hbm,
                 pieces_v, q_recv, q_v, k_v, v_v, scores, heads_v, o_send, o_recv, a_v, wo_v, x_v, rest_v, bo_v,
                 part_v, pair_send, pair_recv, rs_send, rs_recv, y_v, pack_v, q_hot, o_hot, bo_ref, lens_ref,
                 in_sem, k_sem, v_sem, wo_sem, q_ssem, q_rsem, o_ssem, o_rsem, pair_ssem, pair_rsem,
                 rs_ssem, rs_rsem, ag_ssem, ag_rsem, d2d_ssem, d2d_rsem, out_sem):
    me = lax.axis_index('tp')
    local, cache_len, head_dim = k_v.shape
    share = local // PARTS
    rows = share * steps
    per_seq = n * steps
    total = share * per_seq
    depth = a_v.shape[2]
    heads = depth // head_dim
    cols = wo_v.shape[2]
    chips = n // 2
    far = chips // 2
    chip = me // 2
    core = me % 2
    mate = me + 1 - 2 * core
    group = local * n

    barrier = pltpu.get_barrier_semaphore()
    for k in range(1, n):
        pl.semaphore_signal(barrier, inc=1, device_id=peer(lax.rem(me + k, n)), device_id_type=MESH)

    def block_at(index):
        return pl.ds(pl.multiple_of(index * cols, LANES), cols)

    pieces_copy = pltpu.make_async_copy(pieces_hbm, pieces_v, in_sem.at[0])
    pieces_copy.start()
    x_copy = pltpu.make_async_copy(x_hbm.at[:, block_at(me)], x_v, in_sem.at[1])
    x_copy.start()
    bo_copy = pltpu.make_async_copy(bo_hbm, bo_ref, in_sem.at[2])
    bo_copy.start()
    lens_copy = pltpu.make_async_copy(lens_hbm, lens_ref, in_sem.at[3])
    lens_copy.start()

    cache_in = [(pltpu.make_async_copy(k_hbm.at[i], k_v.at[i], k_sem.at[i]),
                 pltpu.make_async_copy(v_hbm.at[i], v_v.at[i], v_sem.at[i])) for i in range(local)]
    for k_copy, v_copy in cache_in:
        k_copy.start()
        v_copy.start()
    offsets = [far]
    for k in range(far - 1, 0, -1):
        offsets += [k, chips - k]
    offsets.append(0)
    wo_copies = []
    for pos, off in enumerate(offsets):
        dest = lax.rem(chip + off, chips)
        for side, dev in enumerate((2 * dest + 1 - core, 2 * dest + core)):
            copy = pltpu.make_async_copy(wo_hbm.at[:, block_at(dev)], wo_v.at[2 * pos + side], wo_sem.at[2 * pos + side])
            copy.start()
            wo_copies.append(copy)

    bo_copy.wait()
    lens_copy.wait()
    bo_v[...] = bo_ref[...].astype(F32)
    tiles = cols // LANES
    bias = jnp.concatenate([bo_v[pl.ds(me * tiles + j, 1), :] for j in range(tiles)], axis=1)
    x_copy.wait()
    row = iota((total, 1), 0)
    for part in range(PARTS):
        source = (row // (n * share)) * group + ((row // share) % n) * local + part * share + row % share
        rest_v[part] = mm(one_hot(total, steps * group, source), x_v[...]) + bias

    def fill(ref, hots):
        for j, hot in enumerate(hots):
            ref[j] = hot

    def held(ref):
        return [ref[j] for j in range(ref.shape[0])]

    fill(q_hot, unpack_hots(
        n, total, heads, lambda row: ((row % per_seq) // steps, (row // per_seq) * steps + row % steps), rows))
    fill(pack_v, pack_hots(
        total, heads, lambda dest, r: (r // steps) * per_seq + dest * steps + r % steps, n, rows))
    fill(o_hot, unpack_hots(
        n, total, heads, lambda row: ((row // share) % n, (row % share) * steps + row // (n * share)), rows))

    def exchange(part, send_buf, recv_buf, send_sem, recv_sem):
        mine = pl.ds(pl.multiple_of(me * PACK, PACK), PACK)
        copies = []
        for k in sorted(range(1, n), key=lambda k: -min(k, n - k)):
            dest = lax.rem(me + k, n)
            copy = pltpu.make_async_remote_copy(
                src_ref=send_buf.at[part, pl.ds(pl.multiple_of(dest * PACK, PACK), PACK)],
                dst_ref=recv_buf.at[part, mine],
                send_sem=send_sem.at[part, k], recv_sem=recv_sem.at[part, k],
                device_id=peer(dest), device_id_type=MESH)
            copy.start()
            copies.append(copy)
        recv_buf[part, mine] = send_buf[part, mine]
        return copies

    pieces_copy.wait()
    pl.semaphore_wait(barrier, n - 1)
    q_copies = [exchange(part, pieces_v, q_recv, q_ssem, q_rsem) for part in range(PARTS)]

    n_rows = heads * per_seq
    factor = head_dim ** -0.5 * 1.4426950408889634
    col_step = iota((n_rows, block), 1) - iota((n_rows, block), 0) % steps

    def fold(value, op):
        out = value[:, :LANES]
        for c in range(1, block // LANES):
            out = op(out, value[:, c * LANES:(c + 1) * LANES])
        return out

    def attend(part):
        for copy in q_copies[part]:
            copy.wait_recv()
        by_head = unpack_rows(q_recv.at[part], held(q_hot), heads, rows)
        for i in range(share):
            for head in range(heads):
                q_v[i, head * per_seq:(head + 1) * per_seq, :] = by_head[head][i * per_seq:(i + 1) * per_seq]

        for copy in cache_in[part * share:(part + 1) * share]:
            copy[0].wait()
            copy[1].wait()

        @pl.loop(0, share)
        def _(i):
            seq = part * share + i
            seq_len = lens_ref[seq]
            q = q_v[i]
            top = jnp.full((n_rows, LANES), -jnp.inf, F32)
            for j in range(cache_len // block):
                at = slice(j * block, (j + 1) * block)
                t = lax.dot_general(q, k_v[seq, at, :], (((1,), (1,)), ((), ())), preferred_element_type=F32)
                t = jnp.where(col_step <= seq_len - j * block, t, -jnp.inf)
                scores[:, at] = t
                top = jnp.maximum(top, fold(t, jnp.maximum))
            top = jnp.max(top, axis=-1, keepdims=True)
            den = jnp.zeros((n_rows, LANES), F32)
            num = jnp.zeros((n_rows, head_dim), F32)
            for j in range(cache_len // block):
                at = slice(j * block, (j + 1) * block)
                p = jnp.exp2((scores[:, at] - top) * factor)
                num = num + mm(p.astype(BF16), v_v[seq, at, :])
                den = den + fold(p, jnp.add)
            out = (num / jnp.sum(den, axis=-1, keepdims=True)).astype(BF16)
            to = pl.ds(pl.multiple_of(i * per_seq, PACK), per_seq)
            for head in range(heads):
                heads_v[to, head * LANES:(head + 1) * LANES] = out[head * per_seq:(head + 1) * per_seq]

        pack_rows(heads_v[...], held(pack_v), heads, rows, o_send.at[part])
        return exchange(part, o_send, o_recv, o_ssem, o_rsem)

    o_copies = [attend(part) for part in range(PARTS)]

    cut = cut_of(total)
    sizes = (cut, total - cut)
    halves = (pl.ds(0, cut), pl.ds(cut, total - cut))
    sign = (-1, 1)
    nexts = [2 * lax.rem(chip + chips + sign[d], chips) + core for d in (0, 1)]
    own = 2 * chip + core
    pair_copies = {}
    arrived = set()
    loaded = set()
    rs_copies = {}
    ag_copies = {}
    d2d_copies = []
    waiting = []
    out_copies = []
    todo = {part: list(offsets) for part in range(PARTS)}

    def collect(part):
        for copy in o_copies[part]:
            copy.wait_recv()
        by_head = unpack_rows(o_recv.at[part], held(o_hot), heads, rows)
        for head in range(heads):
            a_v[part, :, head * LANES:(head + 1) * LANES] = by_head[head]

    def multiply(part, off):
        todo[part].remove(off)
        pos = offsets.index(off)
        first = off not in loaded
        loaded.add(off)
        if first:
            wo_copies[2 * pos].wait()
        pair_send[part, pos] = mm(a_v[part], wo_v[2 * pos]).astype(BF16)
        copy = pltpu.make_async_remote_copy(
            src_ref=pair_send.at[part, pos], dst_ref=pair_recv.at[part, pos], send_sem=pair_ssem.at[part, pos],
            recv_sem=pair_rsem.at[part, pos], device_id=peer(mate), device_id_type=MESH)
        copy.start()
        pair_copies[part, off] = copy
        if first:
            wo_copies[2 * pos + 1].wait()
        part_v[part, pos] = mm(a_v[part], wo_v[2 * pos + 1])

    def chip_sum(part, off, u):
        pos = offsets.index(off)
        if (part, off) not in arrived:
            pair_copies[part, off].wait_recv()
            arrived.add((part, off))
        return part_v[part, pos, halves[u], :] + pair_recv[part, pos, halves[u], :].astype(F32)

    def lone(part, d):
        return d ^ part

    plan = {
        (part, d): [(far, lone(part, d))] + [(k, h) for k in range(far - 1, 0, -1) for h in (1 - lone(part, d), lone(part, d))]
        for part in range(PARTS) for d in (0, 1)}
    n_slots = 2 * far - 1

    def reduce_slot(part, slot):
        for d in (0, 1):
            k, u = plan[part, d][slot]
            value = chip_sum(part, (sign[d] * k) % chips, u)
            if slot >= 2:
                rs_copies[part, d, slot - 2].wait_recv()
                value = value + rs_recv[part, d, slot - 2, :sizes[u], :].astype(F32)
            rs_send[part, d, slot, :sizes[u], :] = value.astype(BF16)
            copy = pltpu.make_async_remote_copy(
                src_ref=rs_send.at[part, d, slot, pl.ds(0, sizes[u])], dst_ref=rs_recv.at[part, d, slot, pl.ds(0, sizes[u])],
                send_sem=rs_ssem.at[part, d, slot], recv_sem=rs_rsem.at[part, d, slot],
                device_id=peer(nexts[d]), device_id_type=MESH)
            copy.start()
            rs_copies[part, d, slot] = copy

    def gather_send(part, d, slot, index, u):
        at = y_v.at[part, index, halves[u]]
        copy = pltpu.make_async_remote_copy(
            src_ref=at, dst_ref=at, send_sem=ag_ssem.at[part, d, slot], recv_sem=ag_rsem.at[part, d, slot],
            device_id=peer(nexts[d]), device_id_type=MESH)
        copy.start()
        ag_copies[part, d, slot] = copy

    def place_out(part, index, sem):
        out = pltpu.make_async_copy(
            y_v.at[part, index], y_hbm.at[pl.ds(part * total, total), block_at(index)], sem)
        out.start()
        out_copies.append(out)

    def spread(part, index, hop):
        at = y_v.at[part, index]
        copy = pltpu.make_async_remote_copy(
            src_ref=at, dst_ref=at, send_sem=d2d_ssem.at[part, hop], recv_sem=d2d_rsem.at[part, hop],
            device_id=peer(mate), device_id_type=MESH)
        copy.start()
        d2d_copies.append(copy)
        waiting.append((copy, part, index + 1 - 2 * core, hop))
        place_out(part, index, out_sem.at[0, part, hop])
        drain(4)

    def drain(left):
        while len(waiting) > left:
            copy, part, other, hop = waiting.pop(0)
            copy.wait_recv()
            place_out(part, other, out_sem.at[1, part, hop])

    def own_step(part):
        for u in (0, 1):
            value = rest_v[part, halves[u], :] + chip_sum(part, 0, u)
            for d in (0, 1):
                slot = n_slots - 1 if lone(part, d) == u else n_slots - 2
                rs_copies[part, d, slot].wait_recv()
                value = value + rs_recv[part, d, slot, :sizes[u], :].astype(F32)
            y_v[part, own, halves[u], :] = value.astype(BF16)
        for slot in (0, 1):
            for d in (0, 1):
                gather_send(part, d, slot, own, lone(part, d) if slot else 1 - lone(part, d))
        spread(part, own, 0)

    landed = {}

    def gather_slot(part, slot):
        for d in (0, 1):
            u = lone(part, d) if slot % 2 else 1 - lone(part, d)
            hop = (-sign[d] * (slot // 2 + 1)) % chips
            index = 2 * lax.rem(chip + hop, chips) + core
            ag_copies[part, d, slot].wait_recv()
            if slot + 2 < n_slots:
                gather_send(part, d, slot + 2, index, u)
            landed[part, hop] = landed.get((part, hop), 0) + 1
            if landed[part, hop] == 2:
                spread(part, index, hop)

    def prepare(part, slot):
        need = [(sign[d] * plan[part, d][slot][0]) % chips for d in (0, 1)] if slot < n_slots else todo[part]
        for off in list(need):
            if off in todo[part]:
                multiply(part, off)

    def step_of(part, s):
        if 0 <= s < n_slots:
            prepare(part, s + 2)
            reduce_slot(part, s)
        elif s == n_slots:
            own_step(part)
        elif n_slots < s <= 2 * n_slots:
            gather_slot(part, s - n_slots - 1)

    lag = 2
    for part in range(PARTS):
        collect(part)
        prepare(part, 0)
        prepare(part, 1)
        if part == 0:
            for s in range(lag):
                step_of(0, s)
    for s in range(lag, 2 * n_slots + 1 + lag):
        for part in range(PARTS):
            step_of(part, s - part * lag)
    drain(0)
    for copies in q_copies + o_copies:
        for copy in copies:
            copy.wait_send()
    for copy in list(pair_copies.values()) + list(rs_copies.values()) + list(ag_copies.values()):
        copy.wait_send()
    for copy in d2d_copies:
        copy.wait_send()
    for out in out_copies:
        out.wait()


def order_kernel(n, y_ref, out_ref, hot_v):
    steps, group, _ = out_ref.shape
    local = group // n
    share = local // PARTS

    @pl.when(pl.program_id(0) == 0)
    def _():
        seq = iota((group, 1), 0)
        dev, i = seq // local, seq % local
        hot_v[...] = one_hot(group, group, (i // share) * (n * share) + dev * share + i % share)

    for s in range(steps):
        src = jnp.concatenate([y_ref[part, s] for part in range(PARTS)], axis=0)
        out_ref[s] = mm(hot_v[...], src).astype(BF16)


def solution(mesh):
    n = mesh.shape['tp']
    anywhere = pl.BlockSpec(memory_space=pl.ANY)
    dma = pltpu.SemaphoreType.DMA

    def in_hbm(array):
        return pltpu.with_memory_space_constraint(array, pltpu.HBM)

    def by_lanes(vector):
        return vector.reshape(-1, LANES)

    def local_block(x_steps, seq_lens, k_cache, v_cache, ln_gain, ln_bias, w_q, b_q, w_kv, b_kv, w_out, b_out):
        steps, group, width = x_steps.shape
        local, cache_len, head_dim = k_cache.shape
        total = steps * group
        q_cols = w_q.shape[1]
        kv_cols = w_kv.shape[1]
        heads = q_cols // head_dim
        per_seq = n * steps
        share = local // PARTS
        piece_cols = -(-share * steps * heads // PACK) * LANES
        piece_shape = (PARTS, n * PACK, piece_cols)
        pieces, k_out, v_out = pl.pallas_call(
            functools.partial(local_kernel, n),
            name='local',
            out_shape=(
                jax.ShapeDtypeStruct(piece_shape, BF16),
                jax.ShapeDtypeStruct(k_cache.shape, BF16),
                jax.ShapeDtypeStruct(v_cache.shape, BF16),
            ),
            in_specs=[anywhere] * 10,
            out_specs=(anywhere, anywhere, anywhere),
            scratch_shapes=[
                pltpu.VMEM((steps, group, width), BF16),
                pltpu.VMEM((total, width), BF16),
                pltpu.VMEM((width, q_cols), BF16),
                pltpu.VMEM((width, kv_cols), BF16),
                pltpu.VMEM(k_cache.shape, BF16),
                pltpu.VMEM(v_cache.shape, BF16),
                pltpu.VMEM((total, q_cols), F32),
                pltpu.VMEM((total, kv_cols), F32),
                pltpu.VMEM((1, width), F32),
                pltpu.VMEM((1, width), F32),
                pltpu.VMEM((1, q_cols), F32),
                pltpu.VMEM((1, kv_cols), F32),
                pltpu.VMEM((local * 8, kv_cols), F32),
                pltpu.VMEM(piece_shape, BF16),
                pltpu.VMEM((width // LANES, LANES), BF16),
                pltpu.VMEM((width // LANES, LANES), BF16),
                pltpu.VMEM((q_cols // LANES, LANES), BF16),
                pltpu.VMEM((kv_cols // LANES, LANES), BF16),
                pltpu.SMEM((local,), jnp.int32),
                dma((steps,)), dma((2,)), dma((2, local)), dma((2, local)), dma((5,)), dma((PARTS,)),
            ],
            compiler_params=pltpu.CompilerParams(vmem_limit_bytes=VMEM_LIMIT),
        )(seq_lens, x_steps, by_lanes(ln_gain), by_lanes(ln_bias), w_q, by_lanes(b_q), w_kv, by_lanes(b_kv), k_cache, v_cache)

        block = cache_len // 3 if cache_len % (3 * LANES) == 0 else cache_len
        cols = width // n
        chips = n // 2
        far = chips // 2
        rows = total // PARTS
        n_pairs = len(pairs_of(heads, share * steps))
        cut = cut_of(rows)
        y = pl.pallas_call(
            functools.partial(group_kernel, n, steps, block),
            name='group',
            out_shape=jax.ShapeDtypeStruct((total, width), BF16),
            in_specs=[anywhere] * 7,
            out_specs=anywhere,
            scratch_shapes=[
                pltpu.VMEM(piece_shape, BF16),
                pltpu.VMEM(piece_shape, BF16),
                pltpu.VMEM((share, heads * per_seq, head_dim), BF16),
                pltpu.VMEM(k_cache.shape, BF16),
                pltpu.VMEM(v_cache.shape, BF16),
                pltpu.VMEM((heads * per_seq, cache_len), F32),
                pltpu.VMEM((rows, q_cols), BF16),
                pltpu.VMEM(piece_shape, BF16),
                pltpu.VMEM(piece_shape, BF16),
                pltpu.VMEM((PARTS, rows, q_cols), BF16),
                pltpu.VMEM((n, q_cols, cols), BF16),
                pltpu.VMEM((total, cols), BF16),
                pltpu.VMEM((PARTS, rows, cols), F32),
                pltpu.VMEM((width // LANES, LANES), F32),
                pltpu.VMEM((PARTS, chips, rows, cols), F32),
                pltpu.VMEM((PARTS, chips, rows, cols), BF16),
                pltpu.VMEM((PARTS, chips, rows, cols), BF16),
                pltpu.VMEM((PARTS, 2, 2 * far - 1, cut, cols), BF16),
                pltpu.VMEM((PARTS, 2, 2 * far - 1, cut, cols), BF16),
                pltpu.VMEM((PARTS, n, rows, cols), BF16),
                pltpu.VMEM((n_pairs, n * PACK, rows), BF16),
                pltpu.VMEM((n_pairs, rows, n * PACK), BF16),
                pltpu.VMEM((n_pairs, rows, n * PACK), BF16),
                pltpu.VMEM((width // LANES, LANES), BF16),
                pltpu.SMEM((local,), jnp.int32),
                dma((4,)), dma((local,)), dma((local,)), dma((n,)),
                dma((PARTS, n)), dma((PARTS, n)), dma((PARTS, n)), dma((PARTS, n)),
                dma((PARTS, chips)), dma((PARTS, chips)),
                dma((PARTS, 2, 2 * far - 1)), dma((PARTS, 2, 2 * far - 1)),
                dma((PARTS, 2, 2 * far - 1)), dma((PARTS, 2, 2 * far - 1)),
                dma((PARTS, chips)), dma((PARTS, chips)), dma((2, PARTS, chips)),
            ],
            compiler_params=pltpu.CompilerParams(
                collective_id=0, has_side_effects=True, vmem_limit_bytes=GROUP_LIMIT),
        )(seq_lens, in_hbm(pieces), in_hbm(k_out), in_hbm(v_out), in_hbm(x_steps.reshape(total, width)), in_hbm(w_out),
          by_lanes(b_out))

        wide = 2 * cols
        y_steps = pl.pallas_call(
            functools.partial(order_kernel, n),
            name='order',
            grid=(width // wide,),
            out_shape=jax.ShapeDtypeStruct(x_steps.shape, BF16),
            in_specs=[pl.BlockSpec((PARTS, steps, group // PARTS, wide), lambda c: (0, 0, 0, c))],
            out_specs=pl.BlockSpec((steps, group, wide), lambda c: (0, 0, c)),
            scratch_shapes=[pltpu.VMEM((group, group), BF16)],
            compiler_params=pltpu.CompilerParams(vmem_limit_bytes=ORDER_LIMIT),
        )(y.reshape(PARTS, steps, group // PARTS, width))
        return y_steps, k_out, v_out

    row_spec = P(('dp', 'tp'), None, None)
    return jax.shard_map(
        local_block,
        mesh=mesh,
        in_specs=(P(None, 'dp', None), P(('dp', 'tp')), row_spec, row_spec, P(None), P(None), P(None, 'tp'), P('tp'), P(None, None), P(None), P('tp', None), P(None)),
        out_specs=(P(None, 'dp', None), row_spec, row_spec),
        check_vma=False,
    )
```

```python
import functools

import jax
import jax.numpy as jnp
from jax import lax
from jax.experimental import pallas as pl
from jax.experimental.pallas import tpu as pltpu
from jax.sharding import PartitionSpec as P

LN_EPS = 1e-5
LANES = 128
PACK = 16
PARTS = 2
VMEM_LIMIT = 60 * 1024 * 1024
GROUP_LIMIT = 44 * 1024 * 1024
ORDER_LIMIT = 16 * 1024 * 1024
MESH = pl.DeviceIdType.MESH
F32 = jnp.float32
BF16 = jnp.bfloat16


def iota(shape, dim):
    return lax.broadcasted_iota(jnp.int32, shape, dim)


def one_hot(rows, cols, index, valid=None):
    at = index if valid is None else jnp.where(valid, index, -1)
    return jnp.where(iota((rows, cols), 1) == at, 1.0, 0.0).astype(BF16)


def mm(a, b):
    return jnp.dot(a, b, preferred_element_type=F32)


def peer(index):
    return {'tp': index}


def tiles_of(head, rows):
    return range(head * rows // PACK, ((head + 1) * rows - 1) // PACK + 1)


def pairs_of(heads, rows):
    return [(tile, head) for head in range(heads) for tile in tiles_of(head, rows)]


def pack_hots(total, heads, source_row, n, rows):
    p = iota((n * PACK, 1), 0)
    dest, slot = p // PACK, p % PACK
    for tile, head in pairs_of(heads, rows):
        unit = tile * PACK + slot
        yield one_hot(n * PACK, total, source_row(dest, unit % rows), unit // rows == head)


def pack_rows(src, hots, heads, rows, send_buf):
    value = {}
    for (tile, head), hot in zip(pairs_of(heads, rows), hots):
        value[tile] = value.get(tile, 0.0) + mm(hot, src[:, head * LANES:(head + 1) * LANES])
    for tile in value:
        send_buf[:, tile * LANES:(tile + 1) * LANES] = value[tile].astype(BF16)


def unpack_hots(n, total, heads, place, rows):
    source, row = place(iota((total, 1), 0))
    for tile, head in pairs_of(heads, rows):
        unit = head * rows + row
        yield one_hot(total, n * PACK, source * PACK + unit % PACK, unit // PACK == tile)


def unpack_rows(recv_buf, hots, heads, rows):
    value = {}
    for (tile, head), hot in zip(pairs_of(heads, rows), hots):
        value[head] = value.get(head, 0.0) + mm(hot, recv_buf[:, tile * LANES:(tile + 1) * LANES])
    return [value[head].astype(BF16) for head in range(heads)]


def cut_of(rows):
    return -(-rows // (2 * PACK)) * PACK


def spread_row(row_ref, src_ref):
    for j in range(src_ref.shape[0]):
        row_ref[:, j * LANES:(j + 1) * LANES] = src_ref[j:j + 1, :].astype(F32)


def local_kernel(n, lens_hbm, x_hbm, gain_hbm, bias_hbm, wq_hbm, bq_hbm, wkv_hbm, bkv_hbm, k_hbm, v_hbm,
                 pieces_hbm, ko_hbm, vo_hbm,
                 x_v, h_v, wq_v, wkv_v, k_v, v_v, acc, kv_acc, gain_v, bias_v, bq_v, bkv_v, fresh,
                 pieces_v, gain_ref, bias_ref, bq_ref, bkv_ref, lens_ref,
                 x_sem, w_sem, in_sem, out_sem, small_sem, piece_sem):
    me = lax.axis_index('tp')
    steps, group, width = x_v.shape
    q_cols = wq_v.shape[1]
    total = steps * group
    local, cache_len, head_dim = k_v.shape
    x_copies = [pltpu.make_async_copy(x_hbm.at[s], x_v.at[s], x_sem.at[s]) for s in range(steps)]
    wkv_copy = pltpu.make_async_copy(wkv_hbm, wkv_v, w_sem.at[0])
    wq_copy = pltpu.make_async_copy(wq_hbm, wq_v, w_sem.at[1])
    caches = ((k_hbm, k_v, ko_hbm), (v_hbm, v_v, vo_hbm))
    ins = [[pltpu.make_async_copy(src.at[i], mid.at[i], in_sem.at[c, i]) for i in range(local)]
           for c, (src, mid, _) in enumerate(caches)]
    outs = [[pltpu.make_async_copy(mid.at[i], dst.at[i], out_sem.at[c, i]) for i in range(local)]
            for c, (_, mid, dst) in enumerate(caches)]
    small = [pltpu.make_async_copy(src, dst, small_sem.at[j]) for j, (src, dst) in enumerate((
        (gain_hbm, gain_ref), (bias_hbm, bias_ref), (bq_hbm, bq_ref), (bkv_hbm, bkv_ref), (lens_hbm, lens_ref)))]
    for copy in x_copies[:1] + small + x_copies[1:] + [wkv_copy, wq_copy]:
        copy.start()
    for copy in ins[0] + ins[1]:
        copy.start(priority=1)
    for copy in small:
        copy.wait()
    spread_row(gain_v, gain_ref)
    spread_row(bias_v, bias_ref)
    spread_row(bq_v, bq_ref)
    spread_row(bkv_v, bkv_ref)

    for s in range(steps):
        x_copies[s].wait()

        @pl.loop(0, group // PACK)
        def _(r):
            at = pl.ds(pl.multiple_of(r * PACK, PACK), PACK)
            x = x_v[s, at, :].astype(F32)
            mean = jnp.mean(x, axis=-1, keepdims=True)
            centered = x - mean
            var = jnp.mean(centered * centered, axis=-1, keepdims=True)
            scaled = centered * lax.rsqrt(var + LN_EPS)
            h = (scaled * gain_v[...] + bias_v[...]).astype(BF16)
            h_v[pl.ds(pl.multiple_of(s * group + r * PACK, PACK), PACK), :] = h

    depth = width // 8

    def product(total_ref, w_v):
        total_ref[...] = jnp.zeros_like(total_ref)

        @pl.loop(0, width // depth)
        def _(c):
            at = pl.ds(pl.multiple_of(c * depth, depth), depth)
            total_ref[...] += mm(h_v[:, at], w_v[at, :])

    wkv_copy.wait()
    product(kv_acc, wkv_v)
    kv = (kv_acc[...] + bkv_v[...]).astype(BF16)
    pad = fresh.shape[0] // local
    row = iota((local * pad, 1), 0)
    fresh[...] = mm(one_hot(local * pad, total, (row % pad) * group + me * local + row // pad, row % pad < steps), kv)
    window = 2 * PACK
    for c in (0, 1):
        for i in range(local):
            mid = caches[c][1]
            seq_len = lens_ref[i]
            start = jnp.minimum((seq_len // PACK) * PACK, cache_len - window)
            at = pl.ds(pl.multiple_of(start, PACK), window)
            pos = iota((window, head_dim), 0) + start
            ins[c][i].wait()
            value = mid[i, at, :].astype(F32)
            for s in range(steps):
                new = fresh[i * pad + s:i * pad + s + 1, c * head_dim:(c + 1) * head_dim]
                value = jnp.where(pos == seq_len + s, new, value)
            mid[i, at, :] = value.astype(BF16)
            outs[c][i].start(priority=1)

    wq_copy.wait()
    product(acc, wq_v)
    q = (acc[...] + bq_v[...]).astype(BF16)
    share = local // PARTS
    pieces = []
    for part in range(PARTS):
        hots = pack_hots(
            total, q_cols // LANES,
            lambda dest, r: (r % steps) * group + dest * local + part * share + r // steps, n, share * steps)
        pack_rows(q, hots, q_cols // LANES, share * steps, pieces_v.at[part])
        piece = pltpu.make_async_copy(pieces_v.at[part], pieces_hbm.at[part], piece_sem.at[part])
        piece.start()
        pieces.append(piece)
    for copy in outs[0] + outs[1] + pieces:
        copy.wait()


def group_kernel(n, steps, block, lens_hbm, pieces_hbm, k_hbm, v_hbm, x_hbm, wo_hbm, bo_hbm, y_hbm,
                 pieces_v, q_recv, q_v, k_v, v_v, scores, heads_v, o_send, o_recv, a_v, wo_v, x_v, rest_v, bo_v,
                 part_v, pair_send, pair_recv, rs_send, rs_recv, y_v, pack_v, q_hot, o_hot, bo_ref, lens_ref, sorted_v, row_hot,
                 in_sem, k_sem, v_sem, wo_sem, q_ssem, q_rsem, o_ssem, o_rsem, pair_ssem, pair_rsem,
                 rs_ssem, rs_rsem, ag_ssem, ag_rsem, d2d_ssem, d2d_rsem, out_sem):
    me = lax.axis_index('tp')
    local, cache_len, head_dim = k_v.shape
    share = local // PARTS
    rows = share * steps
    per_seq = n * steps
    total = share * per_seq
    depth = a_v.shape[2]
    heads = depth // head_dim
    cols = wo_v.shape[2]
    chips = n // 2
    far = chips // 2
    chip = me // 2
    core = me % 2
    mate = me + 1 - 2 * core
    group = local * n

    barrier = pltpu.get_barrier_semaphore()
    for k in range(1, n):
        pl.semaphore_signal(barrier, inc=1, device_id=peer(lax.rem(me + k, n)), device_id_type=MESH)

    def block_at(index):
        return pl.ds(pl.multiple_of(index * cols, LANES), cols)

    pieces_copy = pltpu.make_async_copy(pieces_hbm, pieces_v, in_sem.at[0])
    pieces_copy.start()
    x_copy = pltpu.make_async_copy(x_hbm.at[:, block_at(me)], x_v, in_sem.at[1])
    x_copy.start()
    bo_copy = pltpu.make_async_copy(bo_hbm, bo_ref, in_sem.at[2])
    bo_copy.start()
    lens_copy = pltpu.make_async_copy(lens_hbm, lens_ref, in_sem.at[3])
    lens_copy.start()

    cache_in = [(pltpu.make_async_copy(k_hbm.at[i], k_v.at[i], k_sem.at[i]),
                 pltpu.make_async_copy(v_hbm.at[i], v_v.at[i], v_sem.at[i])) for i in range(local)]
    for k_copy, v_copy in cache_in:
        k_copy.start()
        v_copy.start()
    offsets = [far]
    for k in range(far - 1, 0, -1):
        offsets += [k, chips - k]
    offsets.append(0)
    wo_copies = []
    for pos, off in enumerate(offsets):
        dest = lax.rem(chip + off, chips)
        for side, dev in enumerate((2 * dest + 1 - core, 2 * dest + core)):
            copy = pltpu.make_async_copy(wo_hbm.at[:, block_at(dev)], wo_v.at[2 * pos + side], wo_sem.at[2 * pos + side])
            copy.start()
            wo_copies.append(copy)

    bo_copy.wait()
    lens_copy.wait()
    bo_v[...] = bo_ref[...].astype(F32)
    tiles = cols // LANES
    bias = jnp.concatenate([bo_v[pl.ds(me * tiles + j, 1), :] for j in range(tiles)], axis=1)
    x_copy.wait()
    row = iota((total, 1), 0)
    for part in range(PARTS):
        source = (row // (n * share)) * group + ((row // share) % n) * local + part * share + row % share
        rest_v[part] = mm(one_hot(total, steps * group, source), x_v[...]) + bias

    def fill(ref, hots):
        for j, hot in enumerate(hots):
            ref[j] = hot

    def held(ref):
        return [ref[j] for j in range(ref.shape[0])]

    fill(q_hot, unpack_hots(
        n, total, heads, lambda row: ((row % per_seq) // steps, (row // per_seq) * steps + row % steps), rows))
    fill(pack_v, pack_hots(
        total, heads, lambda dest, r: (r // steps) * per_seq + dest * steps + r % steps, n, rows))
    fill(o_hot, unpack_hots(
        n, total, heads, lambda row: ((row // share) % n, (row % share) * steps + row // (n * share)), rows))

    seq = iota((group, 1), 0)
    row_hot[...] = one_hot(
        group, group, ((seq % local) // share) * (n * share) + (seq // local) * share + seq % share)

    def exchange(part, send_buf, recv_buf, send_sem, recv_sem):
        mine = pl.ds(pl.multiple_of(me * PACK, PACK), PACK)
        copies = []
        for k in sorted(range(1, n), key=lambda k: -min(k, n - k)):
            dest = lax.rem(me + k, n)
            copy = pltpu.make_async_remote_copy(
                src_ref=send_buf.at[part, pl.ds(pl.multiple_of(dest * PACK, PACK), PACK)],
                dst_ref=recv_buf.at[part, mine],
                send_sem=send_sem.at[part, k], recv_sem=recv_sem.at[part, k],
                device_id=peer(dest), device_id_type=MESH)
            copy.start()
            copies.append(copy)
        recv_buf[part, mine] = send_buf[part, mine]
        return copies

    pieces_copy.wait()
    pl.semaphore_wait(barrier, n - 1)
    q_copies = [exchange(part, pieces_v, q_recv, q_ssem, q_rsem) for part in range(PARTS)]

    n_rows = heads * per_seq
    factor = head_dim ** -0.5 * 1.4426950408889634
    col_step = iota((n_rows, block), 1) - iota((n_rows, block), 0) % steps

    def fold(value, op):
        out = value[:, :LANES]
        for c in range(1, block // LANES):
            out = op(out, value[:, c * LANES:(c + 1) * LANES])
        return out

    def attend(part):
        for copy in q_copies[part]:
            copy.wait_recv()
        by_head = unpack_rows(q_recv.at[part], held(q_hot), heads, rows)
        for i in range(share):
            for head in range(heads):
                q_v[i, head * per_seq:(head + 1) * per_seq, :] = by_head[head][i * per_seq:(i + 1) * per_seq]

        for copy in cache_in[part * share:(part + 1) * share]:
            copy[0].wait()
            copy[1].wait()

        @pl.loop(0, share)
        def _(i):
            seq = part * share + i
            seq_len = lens_ref[seq]
            q = q_v[i]
            top = jnp.full((n_rows, LANES), -jnp.inf, F32)
            for j in range(cache_len // block):
                at = slice(j * block, (j + 1) * block)
                t = lax.dot_general(q, k_v[seq, at, :], (((1,), (1,)), ((), ())), preferred_element_type=F32)
                t = jnp.where(col_step <= seq_len - j * block, t, -jnp.inf)
                scores[:, at] = t
                top = jnp.maximum(top, fold(t, jnp.maximum))
            top = jnp.max(top, axis=-1, keepdims=True)
            den = jnp.zeros((n_rows, LANES), F32)
            num = jnp.zeros((n_rows, head_dim), F32)
            for j in range(cache_len // block):
                at = slice(j * block, (j + 1) * block)
                p = jnp.exp2((scores[:, at] - top) * factor)
                num = num + mm(p.astype(BF16), v_v[seq, at, :])
                den = den + fold(p, jnp.add)
            out = (num / jnp.sum(den, axis=-1, keepdims=True)).astype(BF16)
            to = pl.ds(pl.multiple_of(i * per_seq, PACK), per_seq)
            for head in range(heads):
                heads_v[to, head * LANES:(head + 1) * LANES] = out[head * per_seq:(head + 1) * per_seq]

        pack_rows(heads_v[...], held(pack_v), heads, rows, o_send.at[part])
        return exchange(part, o_send, o_recv, o_ssem, o_rsem)

    o_copies = [attend(part) for part in range(PARTS)]

    cut = cut_of(total)
    sizes = (cut, total - cut)
    halves = (pl.ds(0, cut), pl.ds(cut, total - cut))
    sign = (-1, 1)
    nexts = [2 * lax.rem(chip + chips + sign[d], chips) + core for d in (0, 1)]
    own = 2 * chip + core
    pair_copies = {}
    arrived = set()
    loaded = set()
    rs_copies = {}
    ag_copies = {}
    d2d_copies = []
    waiting = []
    halfway = set()
    out_copies = []
    todo = {part: list(offsets) for part in range(PARTS)}

    def collect(part):
        for copy in o_copies[part]:
            copy.wait_recv()
        by_head = unpack_rows(o_recv.at[part], held(o_hot), heads, rows)
        for head in range(heads):
            a_v[part, :, head * LANES:(head + 1) * LANES] = by_head[head]

    def multiply(part, off):
        todo[part].remove(off)
        pos = offsets.index(off)
        first = off not in loaded
        loaded.add(off)
        if first:
            wo_copies[2 * pos].wait()
        pair_send[part, pos] = mm(a_v[part], wo_v[2 * pos]).astype(BF16)
        copy = pltpu.make_async_remote_copy(
            src_ref=pair_send.at[part, pos], dst_ref=pair_recv.at[part, pos], send_sem=pair_ssem.at[part, pos],
            recv_sem=pair_rsem.at[part, pos], device_id=peer(mate), device_id_type=MESH)
        copy.start()
        pair_copies[part, off] = copy
        if first:
            wo_copies[2 * pos + 1].wait()
        part_v[part, pos] = mm(a_v[part], wo_v[2 * pos + 1])

    def chip_sum(part, off, u):
        pos = offsets.index(off)
        if (part, off) not in arrived:
            pair_copies[part, off].wait_recv()
            arrived.add((part, off))
        return part_v[part, pos, halves[u], :] + pair_recv[part, pos, halves[u], :].astype(F32)

    def lone(part, d):
        return d ^ part

    plan = {
        (part, d): [(far, lone(part, d))] + [(k, h) for k in range(far - 1, 0, -1) for h in (1 - lone(part, d), lone(part, d))]
        for part in range(PARTS) for d in (0, 1)}
    n_slots = 2 * far - 1

    def reduce_slot(part, slot):
        for d in (0, 1):
            k, u = plan[part, d][slot]
            value = chip_sum(part, (sign[d] * k) % chips, u)
            if slot >= 2:
                rs_copies[part, d, slot - 2].wait_recv()
                value = value + rs_recv[part, d, slot - 2, :sizes[u], :].astype(F32)
            rs_send[part, d, slot, :sizes[u], :] = value.astype(BF16)
            copy = pltpu.make_async_remote_copy(
                src_ref=rs_send.at[part, d, slot, pl.ds(0, sizes[u])], dst_ref=rs_recv.at[part, d, slot, pl.ds(0, sizes[u])],
                send_sem=rs_ssem.at[part, d, slot], recv_sem=rs_rsem.at[part, d, slot],
                device_id=peer(nexts[d]), device_id_type=MESH)
            copy.start()
            rs_copies[part, d, slot] = copy

    def gather_send(part, d, slot, index, u):
        at = y_v.at[part, index, halves[u]]
        copy = pltpu.make_async_remote_copy(
            src_ref=at, dst_ref=at, send_sem=ag_ssem.at[part, d, slot], recv_sem=ag_rsem.at[part, d, slot],
            device_id=peer(nexts[d]), device_id_type=MESH)
        copy.start()
        ag_copies[part, d, slot] = copy

    def place_out(part, index, side, hop):
        if (side, hop) not in halfway:
            halfway.add((side, hop))
            return
        span = n * share
        for s in range(steps):
            src = jnp.concatenate([y_v[p, index, s * span:(s + 1) * span, :] for p in range(PARTS)], axis=0)
            sorted_v[index, s * group:(s + 1) * group, :] = mm(row_hot[...], src).astype(BF16)
        out = pltpu.make_async_copy(sorted_v.at[index], y_hbm.at[:, block_at(index)], out_sem.at[side, hop])
        out.start()
        out_copies.append(out)

    def spread(part, index, hop):
        at = y_v.at[part, index]
        copy = pltpu.make_async_remote_copy(
            src_ref=at, dst_ref=at, send_sem=d2d_ssem.at[part, hop], recv_sem=d2d_rsem.at[part, hop],
            device_id=peer(mate), device_id_type=MESH)
        copy.start()
        d2d_copies.append(copy)
        waiting.append((copy, part, index + 1 - 2 * core, hop))
        place_out(part, index, 0, hop)
        drain(4)

    def drain(left):
        while len(waiting) > left:
            copy, part, other, hop = waiting.pop(0)
            copy.wait_recv()
            place_out(part, other, 1, hop)

    def own_step(part):
        for u in (0, 1):
            value = rest_v[part, halves[u], :] + chip_sum(part, 0, u)
            for d in (0, 1):
                slot = n_slots - 1 if lone(part, d) == u else n_slots - 2
                rs_copies[part, d, slot].wait_recv()
                value = value + rs_recv[part, d, slot, :sizes[u], :].astype(F32)
            y_v[part, own, halves[u], :] = value.astype(BF16)
        for slot in (0, 1):
            for d in (0, 1):
                gather_send(part, d, slot, own, lone(part, d) if slot else 1 - lone(part, d))
        spread(part, own, 0)

    landed = {}

    def gather_slot(part, slot):
        for d in (0, 1):
            u = lone(part, d) if slot % 2 else 1 - lone(part, d)
            hop = (-sign[d] * (slot // 2 + 1)) % chips
            index = 2 * lax.rem(chip + hop, chips) + core
            ag_copies[part, d, slot].wait_recv()
            if slot + 2 < n_slots:
                gather_send(part, d, slot + 2, index, u)
            landed[part, hop] = landed.get((part, hop), 0) + 1
            if landed[part, hop] == 2:
                spread(part, index, hop)

    def prepare(part, slot):
        need = [(sign[d] * plan[part, d][slot][0]) % chips for d in (0, 1)] if slot < n_slots else todo[part]
        for off in list(need):
            if off in todo[part]:
                multiply(part, off)

    def step_of(part, s):
        if 0 <= s < n_slots:
            prepare(part, s + 2)
            reduce_slot(part, s)
        elif s == n_slots:
            own_step(part)
        elif n_slots < s <= 2 * n_slots:
            gather_slot(part, s - n_slots - 1)

    lag = 2
    for part in range(PARTS):
        collect(part)
        prepare(part, 0)
        prepare(part, 1)
        if part == 0:
            for s in range(lag):
                step_of(0, s)
    for s in range(lag, 2 * n_slots + 1 + lag):
        for part in range(PARTS):
            step_of(part, s - part * lag)
    drain(0)
    for copies in q_copies + o_copies:
        for copy in copies:
            copy.wait_send()
    for copy in list(pair_copies.values()) + list(rs_copies.values()) + list(ag_copies.values()):
        copy.wait_send()
    for copy in d2d_copies:
        copy.wait_send()
    for out in out_copies:
        out.wait()


def emit_kernel(y_hbm, out_hbm, sem):
    pieces = 4
    rows = y_hbm.shape[0] // pieces
    copies = [
        pltpu.make_async_copy(y_hbm.at[pl.ds(j * rows, rows)], out_hbm.at[pl.ds(j * rows, rows)], sem.at[j])
        for j in range(pieces)]
    for copy in copies:
        copy.start()
    for copy in copies:
        copy.wait()


def solution(mesh):
    n = mesh.shape['tp']
    anywhere = pl.BlockSpec(memory_space=pl.ANY)
    dma = pltpu.SemaphoreType.DMA

    def in_hbm(array):
        return pltpu.with_memory_space_constraint(array, pltpu.HBM)

    def by_lanes(vector):
        return vector.reshape(-1, LANES)

    def local_block(x_steps, seq_lens, k_cache, v_cache, ln_gain, ln_bias, w_q, b_q, w_kv, b_kv, w_out, b_out):
        steps, group, width = x_steps.shape
        local, cache_len, head_dim = k_cache.shape
        total = steps * group
        q_cols = w_q.shape[1]
        kv_cols = w_kv.shape[1]
        heads = q_cols // head_dim
        per_seq = n * steps
        share = local // PARTS
        piece_cols = -(-share * steps * heads // PACK) * LANES
        piece_shape = (PARTS, n * PACK, piece_cols)
        pieces, k_out, v_out = pl.pallas_call(
            functools.partial(local_kernel, n),
            name='local',
            out_shape=(
                jax.ShapeDtypeStruct(piece_shape, BF16),
                jax.ShapeDtypeStruct(k_cache.shape, BF16),
                jax.ShapeDtypeStruct(v_cache.shape, BF16),
            ),
            in_specs=[anywhere] * 10,
            out_specs=(anywhere, anywhere, anywhere),
            scratch_shapes=[
                pltpu.VMEM((steps, group, width), BF16),
                pltpu.VMEM((total, width), BF16),
                pltpu.VMEM((width, q_cols), BF16),
                pltpu.VMEM((width, kv_cols), BF16),
                pltpu.VMEM(k_cache.shape, BF16),
                pltpu.VMEM(v_cache.shape, BF16),
                pltpu.VMEM((total, q_cols), F32),
                pltpu.VMEM((total, kv_cols), F32),
                pltpu.VMEM((1, width), F32),
                pltpu.VMEM((1, width), F32),
                pltpu.VMEM((1, q_cols), F32),
                pltpu.VMEM((1, kv_cols), F32),
                pltpu.VMEM((local * 8, kv_cols), F32),
                pltpu.VMEM(piece_shape, BF16),
                pltpu.VMEM((width // LANES, LANES), BF16),
                pltpu.VMEM((width // LANES, LANES), BF16),
                pltpu.VMEM((q_cols // LANES, LANES), BF16),
                pltpu.VMEM((kv_cols // LANES, LANES), BF16),
                pltpu.SMEM((local,), jnp.int32),
                dma((steps,)), dma((2,)), dma((2, local)), dma((2, local)), dma((5,)), dma((PARTS,)),
            ],
            compiler_params=pltpu.CompilerParams(vmem_limit_bytes=VMEM_LIMIT),
        )(seq_lens, x_steps, by_lanes(ln_gain), by_lanes(ln_bias), w_q, by_lanes(b_q), w_kv, by_lanes(b_kv), k_cache, v_cache)

        block = cache_len // 3 if cache_len % (3 * LANES) == 0 else cache_len
        cols = width // n
        chips = n // 2
        far = chips // 2
        rows = total // PARTS
        n_pairs = len(pairs_of(heads, share * steps))
        cut = cut_of(rows)
        y = pl.pallas_call(
            functools.partial(group_kernel, n, steps, block),
            name='group',
            out_shape=jax.ShapeDtypeStruct((total, width), BF16),
            in_specs=[anywhere] * 7,
            out_specs=anywhere,
            scratch_shapes=[
                pltpu.VMEM(piece_shape, BF16),
                pltpu.VMEM(piece_shape, BF16),
                pltpu.VMEM((share, heads * per_seq, head_dim), BF16),
                pltpu.VMEM(k_cache.shape, BF16),
                pltpu.VMEM(v_cache.shape, BF16),
                pltpu.VMEM((heads * per_seq, cache_len), F32),
                pltpu.VMEM((rows, q_cols), BF16),
                pltpu.VMEM(piece_shape, BF16),
                pltpu.VMEM(piece_shape, BF16),
                pltpu.VMEM((PARTS, rows, q_cols), BF16),
                pltpu.VMEM((n, q_cols, cols), BF16),
                pltpu.VMEM((total, cols), BF16),
                pltpu.VMEM((PARTS, rows, cols), F32),
                pltpu.VMEM((width // LANES, LANES), F32),
                pltpu.VMEM((PARTS, chips, rows, cols), F32),
                pltpu.VMEM((PARTS, chips, rows, cols), BF16),
                pltpu.VMEM((PARTS, chips, rows, cols), BF16),
                pltpu.VMEM((PARTS, 2, 2 * far - 1, cut, cols), BF16),
                pltpu.VMEM((PARTS, 2, 2 * far - 1, cut, cols), BF16),
                pltpu.VMEM((PARTS, n, rows, cols), BF16),
                pltpu.VMEM((n_pairs, n * PACK, rows), BF16),
                pltpu.VMEM((n_pairs, rows, n * PACK), BF16),
                pltpu.VMEM((n_pairs, rows, n * PACK), BF16),
                pltpu.VMEM((width // LANES, LANES), BF16),
                pltpu.SMEM((local,), jnp.int32),
                pltpu.VMEM((n, total, cols), BF16),
                pltpu.VMEM((group, group), BF16),
                dma((4,)), dma((local,)), dma((local,)), dma((n,)),
                dma((PARTS, n)), dma((PARTS, n)), dma((PARTS, n)), dma((PARTS, n)),
                dma((PARTS, chips)), dma((PARTS, chips)),
                dma((PARTS, 2, 2 * far - 1)), dma((PARTS, 2, 2 * far - 1)),
                dma((PARTS, 2, 2 * far - 1)), dma((PARTS, 2, 2 * far - 1)),
                dma((PARTS, chips)), dma((PARTS, chips)), dma((2, chips)),
            ],
            compiler_params=pltpu.CompilerParams(
                collective_id=0, has_side_effects=True, vmem_limit_bytes=GROUP_LIMIT),
        )(seq_lens, in_hbm(pieces), in_hbm(k_out), in_hbm(v_out), in_hbm(x_steps.reshape(total, width)), in_hbm(w_out),
          by_lanes(b_out))

        y_steps = pl.pallas_call(
            emit_kernel,
            name='emit',
            out_shape=jax.ShapeDtypeStruct((total, width), BF16),
            in_specs=[anywhere],
            out_specs=anywhere,
            scratch_shapes=[dma((4,))],
            compiler_params=pltpu.CompilerParams(vmem_limit_bytes=ORDER_LIMIT),
        )(y).reshape(x_steps.shape)
        return y_steps, k_out, v_out

    row_spec = P(('dp', 'tp'), None, None)
    return jax.shard_map(
        local_block,
        mesh=mesh,
        in_specs=(P(None, 'dp', None), P(('dp', 'tp')), row_spec, row_spec, P(None), P(None), P(None, 'tp'), P('tp'), P(None, None), P(None), P('tp', None), P(None)),
        out_specs=(P(None, 'dp', None), row_spec, row_spec),
        check_vma=False,
    )
```
